128 devices in a mesh: slab: 32 (over y, x, core), probe: 4 (over z).
Axes of the slice: x: 4, y: 4, z: 4, core: 2. Of those that a mesh axis runs over, the one named last changes fastest.
Arguments:
- probe_fields: bfloat16 [256, 128, 8192], P('probe', 'slab'), may hold values from -6 to 6
- sensor_rows: int32 [4096], replicated, may hold values from 0 to 126, as said below
- sensor_cols: int32 [4096], replicated, may hold values from 0 to 8190
- row_frac: float32 [4096], replicated, may hold values from 0 to 1
- col_frac: float32 [4096], replicated, may hold values from 0 to 1
- sensor_weights: float32 [4096], replicated, may hold values from 0.05 to 1
- owner_order: int32 [4096], replicated, may hold values from 0 to 4095, as said below
Outputs:
- adjoint_sources: bfloat16 [256, 128, 8192], P('probe', 'slab')
- observed: float32 [256, 4096], P('probe', 'slab')
- trace_mean: float32 [], replicated
The draws below stay inside these ranges and needn't reach their ends.
Inputs may be any that keep to these rules, and one draw needn't show every extreme that they name: `sensor_rows`: rows run from 0 to 126. The sensors whose row lies in one slab of 4 rows number at most 512, and some slab holds exactly 512. `owner_order`: A permutation. The 4096 // 32 slots of one owner name at most 16 sensors whose row lies in any one slab, and every owner reaches 16 for some slab.
All inputs are finite; a program needn't handle non-finite values.
Results may differ from the reference program's by a relative error of at most 0.0068.
Values sent between devices are 32-bit elements; how exact they have to be, the bound alone decides.
No kernel may reach another device: no remote copies, remote signals or barrier semaphores. Data moves between devices by JAX's collectives and lax.ppermute only.
A program may use at most 64 MiB of HBM per device.

```python
import math
import jax
import jax.numpy as jnp
from jax import lax

ROWS_DEV = 4
NCOL = 8192
SENSORS = 4096
NX = 128
PROBES = 256


def sensor_layout(key):
    slab_total = NX // ROWS_DEV
    slab_most = 4 * SENSORS // slab_total
    own_count = SENSORS // slab_total
    busiest = jax.random.randint(jax.random.fold_in(key, 11), (), 0, slab_total)
    position = jnp.arange(SENSORS, dtype=jnp.int32)
    others = (position - slab_most) % (slab_total - 1)
    others = others + (others >= busiest).astype(jnp.int32)
    slab_seq = jnp.sort(jnp.where(position < slab_most, busiest, others))
    row_inside = jax.random.randint(jax.random.fold_in(key, 12), (SENSORS,), 0, ROWS_DEV)
    row_inside = jnp.where((slab_seq == slab_total - 1) & (row_inside == ROWS_DEV - 1), row_inside - 1, row_inside)
    rows_seq = (slab_seq * ROWS_DEV + row_inside).astype(jnp.int32)
    sensor_ids = jax.random.permutation(jax.random.fold_in(key, 13), SENSORS).astype(jnp.int32)
    sensor_rows = jnp.zeros((SENSORS,), jnp.int32).at[sensor_ids].set(rows_seq)
    owner_perm = jax.random.permutation(jax.random.fold_in(key, 14), slab_total).astype(jnp.int32)
    shuffle = jax.random.permutation(jax.random.fold_in(key, 15), own_count).astype(jnp.int32)
    rotate = jax.random.randint(jax.random.fold_in(key, 16), (slab_total,), 0, own_count)
    owner_of = owner_perm[position % slab_total]
    inside = (shuffle[position // slab_total] + rotate[owner_of]) % own_count
    slot_of = (owner_of * own_count + inside).astype(jnp.int32)
    owner_order = jnp.zeros((SENSORS,), jnp.int32).at[slot_of].set(sensor_ids)
    return (sensor_rows, owner_order)


def draw_sensor_rows(key, part):
    return sensor_layout(key)[0]


def draw_owner_order(key, part):
    return sensor_layout(key)[1]


def with_ends(result, key, low, top_value):
    longest = result.shape.index(max(result.shape))
    spots = []
    for shift in (0, 1):
        where = [jax.random.randint(jax.random.fold_in(key, axis), (), 0, length) for axis, length in enumerate(result.shape)]
        where[longest] = (where[longest] + shift) % result.shape[longest]
        spots.append(tuple(where))
    return result.at[spots[0]].set(low).at[spots[1]].set(top_value)


def block_levels(rng, dims, split, least, high):
    def one(dim, shards_of):
        steps = jax.random.uniform(jax.random.fold_in(jax.random.fold_in(rng, 6), dim), (shards_of,), jnp.float32, least / len(split), high / len(split))
        return jnp.repeat(jnp.exp(steps), dims[dim] // shards_of).reshape((-1,) + (1,) * (len(dims) - dim - 1))

    loudness = one(*split[0])
    for cut in split[1:]:
        loudness = loudness * one(*cut)
    return loudness


def bell_draw(rng, extent, scale, most, pieces=(), kind=jnp.bfloat16):
    level = block_levels(rng, extent, pieces, -0.22, 0.18) if pieces else 1.0
    entries = jax.random.normal(rng, extent, jnp.float32) * scale * level
    return jnp.minimum(jnp.maximum(entries, -most), most).astype(kind)


def setup_inputs(seed: int = 0) -> dict:
    keys = jax.random.split(jax.random.key(seed), 8)
    return {
        "probe_fields": bell_draw(keys[0], (PROBES, NX, NCOL), 1.0, 6.0, ((0, 4), (1, 32))),
        "sensor_rows": draw_sensor_rows(jax.random.fold_in(keys[7], 71), 0),
        "sensor_cols": with_ends(jax.random.randint(keys[2], (SENSORS,), 0, NCOL - 1), jax.random.fold_in(keys[2], 1), 0, (NCOL - 1) - 1).astype(jnp.int32),
        "row_frac": jnp.clip(jax.random.uniform(keys[3], (SENSORS,), jnp.float32, 0.0, 1.0), 0.0, 1.0),
        "col_frac": jnp.clip(jax.random.uniform(keys[4], (SENSORS,), jnp.float32, 0.0, 1.0), 0.0, 1.0),
        "sensor_weights": jnp.clip(jnp.exp(jax.random.uniform(keys[5], (SENSORS,), jnp.float32, math.log(0.05), math.log(1.0))), 0.05, 1.0),
        "owner_order": draw_owner_order(jax.random.fold_in(keys[7], 71), 0),
    }


def reference(probe_fields, sensor_rows, sensor_cols, row_frac, col_frac, sensor_weights, owner_order):
    rlow = 1.0 - row_frac
    rhigh = row_frac
    clow = lax.optimization_barrier((1.0 - col_frac).astype(jnp.bfloat16)).astype(jnp.float32)
    chigh = lax.optimization_barrier(col_frac.astype(jnp.bfloat16)).astype(jnp.float32)
    rows_next = sensor_rows + 1
    cols_next = sensor_cols + 1

    def sample(field):
        field = field.astype(jnp.float32)
        top = clow * field[sensor_rows, sensor_cols] + chigh * field[sensor_rows, cols_next]
        bottom = clow * field[rows_next, sensor_cols] + chigh * field[rows_next, cols_next]
        return rlow * top + rhigh * bottom

    values = lax.map(sample, probe_fields)
    observed = values[:, owner_order]
    weights = sensor_weights[owner_order]
    spread = observed * weights[None, :]
    trace_mean = jnp.sum(spread * observed) / (PROBES * SENSORS)
    owned_rows = sensor_rows[owner_order]
    owned_cols = sensor_cols[owner_order]
    owned_low = rlow[owner_order]
    owned_high = rhigh[owner_order]
    clow_owned = clow[owner_order]
    chigh_owned = chigh[owner_order]

    def place(spread_row):
        lower = (spread_row * owned_low).astype(jnp.bfloat16).astype(jnp.float32)
        upper = (spread_row * owned_high).astype(jnp.bfloat16).astype(jnp.float32)
        grid = jnp.zeros((NX, NCOL), jnp.float32)
        grid = grid.at[owned_rows, owned_cols].add(lower * clow_owned)
        grid = grid.at[owned_rows, owned_cols + 1].add(lower * chigh_owned)
        grid = grid.at[owned_rows + 1, owned_cols].add(upper * clow_owned)
        grid = grid.at[owned_rows + 1, owned_cols + 1].add(upper * chigh_owned)
        return grid.astype(jnp.bfloat16)

    adjoint_sources = lax.map(place, spread)
    return adjoint_sources, observed, trace_mean
```

```python
import jax
import jax.numpy as jnp
from jax import lax
from jax.experimental import pallas as pl
from jax.experimental.pallas import tpu as pltpu
from jax.sharding import PartitionSpec as P

F32 = jnp.float32
BF16 = jnp.bfloat16
LANES = 128
SLOTS = 16
VMEM_LIMIT = 60 * 2**20


def iota(shape, dim):
    return lax.broadcasted_iota(jnp.int32, shape, dim)


def one_hot(mask):
    return jnp.where(mask, 1.0, 0.0).astype(BF16)


def dot(a, b, dims=((1,), (0,))):
    return lax.dot_general(a, b, (dims, ((), ())), preferred_element_type=F32)


def pieces(x):
    high = x.astype(BF16)
    return high, (x - high.astype(F32)).astype(BF16)


def pieces3(x):
    high = x.astype(BF16)
    rest = x - high.astype(F32)
    mid = rest.astype(BF16)
    return high, mid, (rest - mid.astype(F32)).astype(BF16)


def lookup_rows(order_hi, order_lo, rows):
    out = jnp.zeros(rows.shape, jnp.int32)
    for h in range(rows.shape[0]):
        line = jnp.broadcast_to(rows[h : h + 1, :], rows.shape)
        got = jnp.take_along_axis(line, order_lo, axis=1, mode="promise_in_bounds")
        out = jnp.where(order_hi == h, got, out)
    return out


def slot_lists(slab, owned_rows, order_hi, order_lo, rows, cols, row_frac, col_frac, weights):
    owners = rows.shape[0]
    per_list = owners * SLOTS
    total = 2 * per_list
    upper = one_hot(iota((LANES, LANES), 0) < iota((LANES, LANES), 1))
    lane = iota((owners, per_list), 1)
    owner_of = (lane // 8) % owners == iota((owners, per_list), 0)
    picks = []
    for back in (0, 1):
        match = owned_rows // 4 == slab - back
        rank = dot(one_hot(match), upper)
        ranked = jnp.where(match, rank, -1.0).astype(BF16)
        spread_rank = dot(ranked, one_hot(owner_of), ((0,), (0,)))
        place = iota((1, per_list), 1)
        place = ((place // (8 * owners)) * 8 + place % 8).astype(F32)
        picks.append(jnp.where(spread_rank == place, 1.0, 0.0))
    pick = jnp.concatenate(picks, axis=1)
    present = jnp.sum(pick, axis=0, keepdims=True)
    pick = pick.astype(BF16)
    owner_mask = jnp.concatenate([jnp.where(owner_of, 1.0, 0.0)] * 2, axis=1)
    ids = jnp.concatenate([order_hi, order_lo], axis=0).astype(F32).astype(BF16)
    got = dot(ids, pick)
    id_hi = jnp.sum(got[:owners] * owner_mask, axis=0, keepdims=True)
    id_lo = jnp.sum(got[owners:] * owner_mask, axis=0, keepdims=True)
    lo_iota = iota((LANES, total), 0).astype(F32)
    low_pick = jnp.where(lo_iota == id_lo, present, 0.0).astype(BF16)
    hi_mask = jnp.where(iota((owners, total), 0).astype(F32) == id_hi, 1.0, 0.0)
    table = [rows.astype(F32).astype(BF16), (cols // LANES).astype(F32).astype(BF16), (cols % LANES).astype(F32).astype(BF16)]
    table += list(pieces(row_frac))
    table += [(1.0 - col_frac).astype(BF16), col_frac.astype(BF16)]
    table += list(pieces(weights))
    got = dot(jnp.concatenate(table, axis=0), low_pick)
    field = [jnp.sum(got[owners * n : owners * (n + 1)] * hi_mask, axis=0, keepdims=True) for n in range(len(table))]
    row, tile, inner, frac, clow, chigh, weight = (
        field[0], field[1], field[2], field[3] + field[4], field[5], field[6], field[7] + field[8],
    )
    local = (slab * 4).astype(F32)
    sides = []
    for r in range(4):
        here = local + r
        sides.append(jnp.where(row == here, 1.0 - frac, jnp.where(row + 1.0 == here, frac, 0.0)))
    return tile, inner, clow, chigh, sides, weight


def column_parts(inner, clow, chigh):
    count = inner.shape[1]
    cell = iota((LANES, count), 0).astype(F32)
    main = jnp.where(cell == inner, clow, jnp.where(cell == inner + 1.0, chigh, 0.0)).astype(BF16)
    first = iota((16, count), 0) == 0
    carry = jnp.where(first & (inner == LANES - 1.0), chigh, 0.0).astype(BF16)
    return main, carry


def column_table(number, tile, main, carry):
    one = jnp.ones((), BF16)
    zero = jnp.zeros((), BF16)
    is_tile = [jnp.where(tile == float(2 * number + k), one, zero) for k in (-1, 0, 1)]
    parts = []
    for k in (0, 1):
        parts.append(main[:16] * is_tile[k + 1] + carry * is_tile[k])
        for g in range(1, 8):
            parts.append(main[16 * g : 16 * g + 16] * is_tile[k + 1])
    return jnp.concatenate(parts, axis=0)


def sum_matrix():
    return one_hot(iota((64, 256), 0) == iota((64, 256), 1) // 4)


def forward_kernel(slab_ref, rows_ref, cols_ref, rf_ref, cf_ref, w_ref, order_ref, u_ref, part_ref, meta_ref, place_ref, scr, sem):
    chunks = 8
    width = scr.shape[1] // chunks

    def copy(c, k):
        where = pl.ds(c * width, width)
        return pltpu.make_async_copy(u_ref.at[:, k, where], scr.at[:, where, pl.ds(4 * k, 4)], sem.at[c, k])

    for c in range(chunks):
        for k in range(4):
            copy(c, k).start()
    slab = slab_ref[0]
    order = order_ref[...]
    order_hi = order // LANES
    order_lo = order % LANES
    rows = rows_ref[...]
    owned_rows = lookup_rows(order_hi, order_lo, rows)
    tile, inner, clow, chigh, sides, weight = slot_lists(
        slab, owned_rows, order_hi, order_lo, rows, cols_ref[...], rf_ref[...], cf_ref[...], w_ref[...]
    )
    zero = jnp.zeros_like(tile)
    meta_ref[...] = jnp.concatenate([tile, inner, clow, chigh] + sides + [weight] + [zero] * 7, axis=0)
    own = jnp.sum(jnp.where(iota(owned_rows.shape, 0) == slab, owned_rows // 4, 0).astype(F32), axis=0, keepdims=True)
    across = jnp.broadcast_to(own, (LANES, LANES))
    before = (across == across.T) & (iota((LANES, LANES), 0) < iota((LANES, LANES), 1))
    rank = jnp.sum(jnp.where(before, 1.0, 0.0), axis=0, keepdims=True)
    half = jnp.where(rank >= 8.0, 1.0, 0.0)
    place_ref[...] = jnp.concatenate([own * 8.0 + rank - 8.0 * half, half] + [jnp.zeros_like(own)] * 6, axis=0)
    main, carry = column_parts(inner, clow, chigh)
    tile16 = jnp.broadcast_to(tile, (16, tile.shape[1])).astype(BF16)
    total = tile.shape[1]
    acc = jnp.zeros((256, total), F32)
    for c in range(chunks):
        for k in range(4):
            copy(c, k).wait()
        for n in range(c * width // 2, (c + 1) * width // 2):
            fields = jnp.concatenate([scr[:, 2 * n].reshape(256, LANES), scr[:, 2 * n + 1].reshape(256, LANES)], axis=1)
            acc = acc + dot(fields, column_table(n, tile16, main, carry))
    side = jnp.concatenate(sides * 2, axis=0)
    weighted = acc * jnp.tile(side, (32, 1))
    high, low = pieces(weighted)
    gather = sum_matrix()
    part_ref[...] = dot(gather, high) + dot(gather, low)


def combine_kernel(part_ref, above_ref, below_ref, meta_ref, probe_ref, send_ref, src_ref):
    count = above_ref.shape[1]
    value = part_ref[:, :count] + above_ref[...]
    before = part_ref[:, count:] + below_ref[...]
    weight = meta_ref[8:9, :]
    spread = jnp.concatenate([value, before], axis=1) * weight
    squares = jnp.sum(spread[:, :count] * value, axis=0, keepdims=True)
    trace = jnp.sum(squares, axis=1, keepdims=True)
    probe = probe_ref[0]
    groups = 4
    send_ref[...] = jnp.broadcast_to(trace, send_ref.shape)
    half = count // 2
    stacked = jnp.concatenate([value[:, :half], value[:, half:]], axis=0)
    blocks = stacked.T
    for o in range(half // 8):
        send_ref[pl.ds(9 * (groups * o + probe), 8), :] = blocks[8 * o : 8 * o + 8]
    repeat = one_hot(iota((256, 64), 0) // 4 == iota((256, 64), 1))
    tall = dot(repeat, spread.astype(BF16))
    side = jnp.concatenate([meta_ref[4:8, :]] * 2, axis=0)
    src_ref[...] = (tall * jnp.tile(side, (32, 1))).astype(BF16)


def adjoint_kernel(src_ref, meta_ref, out_ref, scr, sem):
    chunks = 8
    width = scr.shape[1] // chunks

    def copy(c, k):
        where = pl.ds(c * width, width)
        return pltpu.make_async_copy(scr.at[:, where, pl.ds(4 * k, 4)], out_ref.at[:, k, where], sem.at[c, k])

    tile, inner, clow, chigh = (meta_ref[n : n + 1, :] for n in range(4))
    main, carry = column_parts(inner, clow, chigh)
    tile16 = jnp.broadcast_to(tile, (16, tile.shape[1])).astype(BF16)
    sources = src_ref[...]
    for c in range(chunks):
        for n in range(c * width // 2, (c + 1) * width // 2):
            cells = dot(sources, column_table(n, tile16, main, carry), ((1,), (1,))).astype(BF16)
            scr[:, 2 * n] = cells[:, :LANES].reshape(16, 16, LANES)
            scr[:, 2 * n + 1] = cells[:, LANES:].reshape(16, 16, LANES)
        for k in range(4):
            copy(c, k).start()
    for c in range(chunks):
        for k in range(4):
            copy(c, k).wait()


def finish_kernel(got_ref, place_ref, probe_ref, observed_ref, total_ref):
    probe = probe_ref[0]
    groups = 4
    values = jnp.concatenate([got_ref[pl.ds(9 * (groups * q + probe), 8), :] for q in range(32)], axis=0)
    pick = one_hot(iota((256, LANES), 0).astype(F32) == place_ref[0:1, :])
    found = sum(dot(part, pick, ((0,), (0,))) for part in pieces3(values))
    observed_ref[...] = jnp.where(place_ref[1:2, :] > 0.5, found[64:], found[:64])
    traces = got_ref[pl.ds(8, 128, stride=9), :]
    total_ref[...] = jnp.broadcast_to(jnp.sum(traces, axis=0, keepdims=True), (8, LANES))


def call(kernel, inputs, spaces, outs, scratch=(), out_spaces=None):
    vmem, smem, anywhere = pltpu.VMEM, pltpu.SMEM, pl.ANY
    kinds = {"v": vmem, "s": smem, "h": anywhere}
    return pl.pallas_call(
        kernel,
        in_specs=[pl.BlockSpec(memory_space=kinds[k]) for k in spaces],
        out_specs=[pl.BlockSpec(memory_space=kinds[k]) for k in out_spaces or "v" * len(outs)],
        out_shape=[jax.ShapeDtypeStruct(*o) for o in outs],
        scratch_shapes=list(scratch),
        compiler_params=pltpu.CompilerParams(vmem_limit_bytes=VMEM_LIMIT),
        name=kernel.__name__,
    )(*inputs)


def body(probe_fields, sensor_rows, sensor_cols, row_frac, col_frac, sensor_weights, owner_order):
    slab = lax.axis_index("slab").astype(jnp.int32).reshape(1)
    probe = lax.axis_index("probe").astype(jnp.int32).reshape(1)
    slabs = lax.axis_size("slab")
    devices = slabs * lax.axis_size("probe")
    per_list = slabs * SLOTS
    tiles = probe_fields.shape[2] // LANES
    fields = probe_fields.reshape(16, 4, 4, tiles, LANES).transpose(0, 1, 3, 2, 4)
    flat = [x.reshape(slabs, LANES) for x in (sensor_rows, sensor_cols, row_frac, col_frac, sensor_weights, owner_order)]
    part, meta, place = call(
        forward_kernel,
        [slab] + flat + [fields],
        "svvvvvvh",
        [((64, 2 * per_list), F32), ((16, 2 * per_list), F32), ((8, LANES), F32)],
        [pltpu.VMEM((16, tiles, 16, LANES), BF16), pltpu.SemaphoreType.DMA((8, 4))],
    )
    up = [(i, i + 1) for i in range(slabs - 1)]
    down = [(i + 1, i) for i in range(slabs - 1)]
    below = lax.ppermute(part[:, :per_list], "slab", up)
    above = lax.ppermute(part[:, per_list:], "slab", down)
    send, sources = call(
        combine_kernel,
        [part, above, below, meta, probe],
        "vvvvs",
        [((9 * devices, LANES), F32), ((256, 2 * per_list), BF16)],
    )
    got = lax.all_to_all(send.reshape(devices, 1, 9 * LANES), ("slab", "probe"), 0, 0, tiled=True)
    (out,) = call(
        adjoint_kernel,
        [sources, meta],
        "vv",
        [(fields.shape, BF16)],
        [pltpu.VMEM((16, tiles, 16, LANES), BF16), pltpu.SemaphoreType.DMA((8, 4))],
        "h",
    )
    observed, total = call(
        finish_kernel,
        [got.reshape(9 * devices, LANES), place, probe],
        "vvs",
        [((64, LANES), F32), ((8, LANES), F32)],
    )
    adjoint = out.transpose(0, 1, 3, 2, 4).reshape(probe_fields.shape)
    count = probe_fields.shape[0] * lax.axis_size("probe") * sensor_rows.shape[0]
    return adjoint, observed, total[0, 0] / count


def solution(mesh):
    placed = (P("probe", "slab", None), P(), P(), P(), P(), P(), P())
    return jax.shard_map(
        body,
        mesh=mesh,
        in_specs=placed,
        out_specs=(P("probe", "slab", None), P("probe", "slab"), P()),
        check_vma=False,
    )
```

```python
import functools

import jax
import jax.numpy as jnp
from jax import lax
from jax.experimental import pallas as pl
from jax.experimental.pallas import tpu as pltpu
from jax.sharding import PartitionSpec as P

F32 = jnp.float32
BF16 = jnp.bfloat16
LANES = 128
SLOTS = 16
VMEM_LIMIT = 60 * 2**20
CHUNKS = 1
OUT_CHUNKS = 8


def iota(shape, dim):
    return lax.broadcasted_iota(jnp.int32, shape, dim)


def one_hot(mask):
    return jnp.where(mask, 1.0, 0.0).astype(BF16)


def dot(a, b, dims=((1,), (0,))):
    return lax.dot_general(a, b, (dims, ((), ())), preferred_element_type=F32)


def pieces(x):
    high = x.astype(BF16)
    return high, (x - high.astype(F32)).astype(BF16)


def pieces3(x):
    high = x.astype(BF16)
    rest = x - high.astype(F32)
    mid = rest.astype(BF16)
    return high, mid, (rest - mid.astype(F32)).astype(BF16)


def lookup_rows(order_hi, order_lo, rows):
    out = jnp.zeros(rows.shape, jnp.int32)
    for h in range(rows.shape[0]):
        line = jnp.broadcast_to(rows[h : h + 1, :], rows.shape)
        got = jnp.take_along_axis(line, order_lo, axis=1, mode="promise_in_bounds")
        out = jnp.where(order_hi == h, got, out)
    return out


def owner_slots(slab, owned_rows):
    upper = one_hot(iota((LANES, LANES), 0) < iota((LANES, LANES), 1))
    match = owned_rows // 4 == slab
    last = match & (owned_rows % 4 == 3)
    rank = dot(one_hot(match & ~last), upper)
    back_rank = dot(one_hot(last), upper)
    many = jnp.max(jnp.where(last & (back_rank > 7.5), 1.0, 0.0))
    return jnp.where(last, SLOTS - 1.0 - back_rank, jnp.where(match, rank, -1.0)).astype(BF16), many


def slot_fields(slab, slots, pieces_of, order_hi, order_lo, rows, cols, row_frac, col_frac, weights):
    owners = rows.shape[0]
    part = owners * 8
    lanes = iota((owners, part), 1)
    owner_of = one_hot((lanes // 8) % owners == iota((owners, part), 0))
    spread = [dot(x, owner_of, ((0,), (0,))) for x in slots]
    place = (iota((1, part), 1) % 8).astype(F32)
    pick = jnp.concatenate([jnp.where(spread[q] == place + 8.0 * half, 1.0, 0.0) for q, half in pieces_of], axis=1)
    present = jnp.sum(pick, axis=0, keepdims=True)
    total = pick.shape[1]
    owner_mask = jnp.concatenate([owner_of.astype(F32)] * len(pieces_of), axis=1)
    ids = jnp.concatenate([order_hi, order_lo], axis=0).astype(F32).astype(BF16)
    got = dot(ids, pick.astype(BF16))
    id_hi = jnp.sum(got[:owners] * owner_mask, axis=0, keepdims=True)
    id_lo = jnp.sum(got[owners:] * owner_mask, axis=0, keepdims=True)
    lo_iota = iota((LANES, total), 0).astype(F32)
    low_pick = jnp.where(lo_iota == id_lo, present, 0.0).astype(BF16)
    hi_mask = jnp.where(iota((owners, total), 0).astype(F32) == id_hi, 1.0, 0.0)
    table = [rows.astype(F32).astype(BF16), (cols // LANES).astype(F32).astype(BF16), (cols % LANES).astype(F32).astype(BF16)]
    table += list(pieces(row_frac))
    table += [(1.0 - col_frac).astype(BF16), col_frac.astype(BF16)]
    table += list(pieces(weights))
    got = dot(jnp.concatenate(table, axis=0), low_pick)
    field = [jnp.sum(got[owners * n : owners * (n + 1)] * hi_mask, axis=0, keepdims=True) for n in range(len(table))]
    row, tile, inner, frac, clow, chigh, weight = (
        field[0], field[1], field[2], field[3] + field[4], field[5], field[6], field[7] + field[8],
    )
    local = (slab * 4).astype(F32)
    sides = []
    for r in range(4):
        here = local + r
        sides.append(jnp.where(row == here, 1.0 - frac, jnp.where(row + 1.0 == here, frac, 0.0)))
    return jnp.concatenate([tile, inner, clow, chigh] + sides + [weight] + [jnp.zeros_like(tile)] * 7, axis=0)


def column_parts(meta):
    tile, inner, clow, chigh = (meta[n : n + 1] for n in range(4))
    count = inner.shape[1]
    cell = iota((LANES, count), 0).astype(F32)
    main = jnp.where(cell == inner, clow, jnp.where(cell == inner + 1.0, chigh, 0.0)).astype(BF16)
    first = iota((16, count), 0) == 0
    carry = jnp.where(first & (inner == LANES - 1.0), chigh, 0.0).astype(BF16)
    return main, carry, jnp.broadcast_to(tile, (16, count)).astype(BF16)


def row_sides(meta):
    return jnp.tile(jnp.concatenate([meta[4:8]] * 2, axis=0), (32, 1))


def column_table(number, tile, main, carry):
    one = jnp.ones((), BF16)
    zero = jnp.zeros((), BF16)
    first = 2.0 * number if isinstance(number, int) else 2.0 * number.astype(F32)
    is_tile = [jnp.where(tile == first + k, 1.0, 0.0).astype(BF16) if tile.dtype == F32 else jnp.where(tile == first + k, one, zero) for k in (-1, 0, 1)]
    parts = []
    for k in (0, 1):
        parts.append(main[:16] * is_tile[k + 1] + carry * is_tile[k])
        for g in range(1, 8):
            parts.append(main[16 * g : 16 * g + 16] * is_tile[k + 1])
    return jnp.concatenate(parts, axis=0)


def row_sum(x, group):
    count = x.shape[0] // group
    gather = one_hot(iota((count, x.shape[0]), 0) == iota((count, x.shape[0]), 1) // group)
    high, low = pieces(x)
    return dot(gather, high) + dot(gather, low)


def to_blocks(value):
    half = value.shape[1] // 2
    return jnp.concatenate([value[:, :half], value[:, half:]], axis=0).T


def field_block(scr, n):
    return jnp.concatenate([scr[:, 2 * n + m].reshape(256, LANES) for m in (0, 1)], axis=1)


def forward_kernel(
    slab_ref, rows_hbm, cols_hbm, rf_hbm, cf_hbm, w_hbm, order_hbm, u_ref,
    own_ref, last_ref, same_ref, cross_ref, meta_ref, place_ref, flag_ref,
    scr, small_i, small_f, sem, small_sem,
):
    chunks = CHUNKS
    width = scr.shape[1] // chunks

    def copy(c, k):
        where = pl.ds(c * width, width)
        return pltpu.make_async_copy(u_ref.at[:, k, where], scr.at[:, where, pl.ds(4 * k, 4)], sem.at[c, k])

    small = [
        pltpu.make_async_copy(src, dst, small_sem.at[n])
        for n, (src, dst) in enumerate(
            [(order_hbm, small_i.at[0]), (rows_hbm, small_i.at[1]), (cols_hbm, small_i.at[2])]
            + [(rf_hbm, small_f.at[0]), (cf_hbm, small_f.at[1]), (w_hbm, small_f.at[2])]
        )
    ]
    for x in small:
        x.start()
    for c in range(chunks):
        for k in range(4):
            copy(c, k).start()
    for x in small:
        x.wait()
    slab = slab_ref[0]
    order = small_i[0]
    order_hi = order // LANES
    order_lo = order % LANES
    rows = small_i[1]
    owned_rows = lookup_rows(order_hi, order_lo, rows)
    count = own_ref.shape[1]
    skip = count // 2
    given = (order_hi, order_lo, rows, small_i[2], small_f[0], small_f[1], small_f[2])
    own_slots, _ = owner_slots(slab, owned_rows)
    last_slots, many = owner_slots(slab - 1, owned_rows)
    flag_ref[0] = (many > 0.5).astype(jnp.int32)
    meta = slot_fields(slab, (own_slots, last_slots), ((0, 0), (0, 1), (1, 1)), *given)
    meta_ref[:, :count] = meta[:, :count]
    meta_ref[:, count : count + skip] = jnp.zeros((16, skip), F32)
    meta_ref[:, count + skip :] = meta[:, count:]
    own_rows = jnp.sum(jnp.where(iota(owned_rows.shape, 0) == slab, owned_rows, 0).astype(F32), axis=0, keepdims=True)
    own = jnp.floor(own_rows * 0.25)
    on_last = jnp.where(own_rows - own * 4.0 == 3.0, 1.0, 0.0)
    kind = jnp.broadcast_to(own * 2.0 + on_last, (LANES, LANES))
    before = (kind == kind.T) & (iota((LANES, LANES), 0) < iota((LANES, LANES), 1))
    rank = jnp.sum(jnp.where(before, 1.0, 0.0), axis=0, keepdims=True)
    rank = jnp.where(on_last > 0.5, SLOTS - 1.0 - rank, rank)
    half = jnp.where(rank >= 8.0, 1.0, 0.0)
    place_ref[...] = jnp.concatenate([own * 8.0 + rank - 8.0 * half, half] + [jnp.zeros_like(own)] * 6, axis=0)
    main, carry, tile16 = column_parts(meta)
    sums = [jnp.zeros((256, count), F32)] + [jnp.zeros((128, skip), F32)] * 2
    for c in range(chunks):
        for k in range(4):
            copy(c, k).wait()
        for n in range(c * width // 2, (c + 1) * width // 2):
            block = field_block(scr, n)
            table = column_table(n, tile16, main, carry)
            sums[0] = sums[0] + dot(block, table[:, :count])
            for m in (0, 1):
                sums[1 + m] = sums[1 + m] + dot(block[128 * m : 128 * m + 128], table[:, count:])
    acc = jnp.concatenate([sums[0], jnp.concatenate(sums[1:], axis=0)], axis=1)
    part = row_sum(acc * row_sides(meta), 4)
    even = slab % 2 == 0

    def give(own_part, last_part):
        last_ref[...] = last_part
        same_ref[...] = jnp.where(even, own_part, last_part)
        cross_ref[...] = jnp.where(even, last_part, own_part)

    own_ref[...] = part[:, :count]
    give(part[:, :count], jnp.concatenate([jnp.zeros((64, skip), F32), part[:, count:]], axis=1))

    @pl.when(flag_ref[0] != 0)
    def _():
        order = small_i[0]
        order_hi = order // LANES
        order_lo = order % LANES
        rows = small_i[1]
        slots, _ = owner_slots(slab - 1, lookup_rows(order_hi, order_lo, rows))
        given = (order_hi, order_lo, rows, small_i[2], small_f[0], small_f[1], small_f[2])
        far_meta = slot_fields(slab, (slots,), ((0, 0),), *given)
        meta_ref[:, count : count + skip] = far_meta
        far_main, far_carry, _ = column_parts(far_meta)
        far_tile = jnp.broadcast_to(far_meta[:1], (16, skip))

        def step(n, far):
            return far + dot(field_block(scr, n), column_table(n, far_tile, far_main, far_carry))

        far = lax.fori_loop(0, scr.shape[1] // 2, step, jnp.zeros((256, skip), F32))
        give(own_ref[...], jnp.concatenate([row_sum(far * row_sides(far_meta), 4), last_ref[:, skip:]], axis=1))


def combine_kernel(own_ref, last_ref, same_ref, cross_ref, meta_ref, at_ref, block_ref, trace_ref, src_ref):
    count = own_ref.shape[1]
    even = at_ref[0] % 2 == 0
    same = same_ref[...]
    cross = cross_ref[...]
    value = own_ref[...] + jnp.where(even, same, cross)
    before = last_ref[...] + jnp.where(even, cross, same)
    weight = meta_ref[8:9, :]
    spread = jnp.concatenate([value, before], axis=1) * weight
    squares = jnp.sum(spread[:, :count] * value, axis=0, keepdims=True)
    trace = jnp.sum(squares, axis=1, keepdims=True)
    lines = to_blocks(value)
    block_ref[...] = lines
    trace_ref[...] = jnp.broadcast_to(trace, trace_ref.shape)
    repeat = one_hot(iota((256, 64), 0) // 4 == iota((256, 64), 1))
    tall = dot(repeat, spread.astype(BF16))
    src_ref[...] = (tall * row_sides(meta_ref[...])).astype(BF16)


def adjoint_kernel(src_ref, meta_ref, flag_ref, out_ref, scr, sem):
    chunks = OUT_CHUNKS
    width = scr.shape[1] // chunks

    def copy(c, k):
        return pltpu.make_async_copy(
            scr.at[:, pl.ds(c * width, width), pl.ds(4 * k, 4)], out_ref.at[:, k, pl.ds(c * width, width)], sem.at[c, k]
        )

    def spread_all(keep):
        main, carry, tile16 = column_parts(keep(meta_ref[...]))
        sources = keep(src_ref[...])
        for c in range(chunks):
            for n in range(c * width // 2, (c + 1) * width // 2):
                table = column_table(n, tile16, main, carry)
                cells = dot(sources, table, ((1,), (1,))).astype(BF16)
                scr[:, 2 * n] = cells[:, :LANES].reshape(16, 16, LANES)
                scr[:, 2 * n + 1] = cells[:, LANES:].reshape(16, 16, LANES)
            for k in range(4):
                copy(c, k).start()

    count = meta_ref.shape[1] // 2

    @pl.when(flag_ref[0] == 0)
    def _():
        spread_all(lambda x: jnp.concatenate([x[:, :count], x[:, count + count // 2 :]], axis=1))

    @pl.when(flag_ref[0] != 0)
    def _():
        spread_all(lambda x: x)

    for c in range(chunks):
        for k in range(4):
            copy(c, k).wait()


def pack_kernel(block_ref, *refs):
    *trace_refs, send_ref = refs
    trace = sum(ref[...] for ref in trace_refs)[:1, :]
    for o in range(block_ref.shape[0] // 8):
        send_ref[9 * o : 9 * o + 8, :] = block_ref[8 * o : 8 * o + 8, :]
        send_ref[9 * o + 8 : 9 * o + 9, :] = trace


def finish_kernel(got_ref, place_ref, observed_ref, total_ref, *, scale):
    slabs = got_ref.shape[0] // 9
    values = jnp.concatenate([got_ref[9 * q : 9 * q + 8, :] for q in range(slabs)], axis=0)
    pick = one_hot(iota((8 * slabs, LANES), 0).astype(F32) == place_ref[0:1, :])
    found = sum(dot(part, pick, ((0,), (0,))) for part in pieces3(values))
    observed_ref[...] = jnp.where(place_ref[1:2, :] > 0.5, found[64:], found[:64])
    traces = jnp.sum(got_ref[pl.ds(8, slabs, stride=9), :], axis=0, keepdims=True)
    total_ref[...] = traces[:, :1] * scale


def call(kernel, inputs, outs, scratch=(), **params):
    kinds = {"v": pltpu.VMEM, "s": pltpu.SMEM, "h": pl.ANY, "w": pltpu.VMEM}
    arrays = [pltpu.with_memory_space_constraint(x, pltpu.VMEM) if k == "w" else x for k, x in inputs]
    return pl.pallas_call(
        functools.partial(kernel, **params),
        in_specs=[pl.BlockSpec(memory_space=kinds[k]) for k, _ in inputs],
        out_specs=[pl.BlockSpec(memory_space=kinds[k]) for k, _, _ in outs],
        out_shape=[pltpu.VMEM(s, t) if k == "w" else jax.ShapeDtypeStruct(s, t) for k, s, t in outs],
        scratch_shapes=list(scratch),
        compiler_params=pltpu.CompilerParams(vmem_limit_bytes=VMEM_LIMIT),
    )(*arrays)


def body(probe_fields, sensor_rows, sensor_cols, row_frac, col_frac, sensor_weights, owner_order):
    at = lax.axis_index("slab").astype(jnp.int32).reshape(1)
    slabs = lax.axis_size("slab")
    groups = lax.axis_size("probe")
    per_list = slabs * SLOTS
    tiles = probe_fields.shape[2] // LANES
    fields = probe_fields.reshape(16, 4, 4, tiles, LANES).transpose(0, 1, 3, 2, 4)
    flat = [x.reshape(slabs, LANES) for x in (sensor_rows, sensor_cols, row_frac, col_frac, sensor_weights, owner_order)]
    own, last, to_same, to_cross, meta, place, flag = call(
        forward_kernel,
        [("s", at)] + [("h", x) for x in flat] + [("h", fields)],
        [("w", (64, per_list), F32)] * 4
        + [("w", (16, 2 * per_list), F32), ("w", (8, LANES), F32), ("s", (1,), jnp.int32)],
        [
            pltpu.VMEM((16, tiles, 16, LANES), BF16),
            pltpu.VMEM((3, slabs, LANES), jnp.int32),
            pltpu.VMEM((3, slabs, LANES), F32),
            pltpu.SemaphoreType.DMA((CHUNKS, 4)),
            pltpu.SemaphoreType.DMA((6,)),
        ],
    )
    swap_cross = [(i, i + 1 if i % 2 else i - 1) for i in range(1, slabs - 1)]
    swap_same = [(i, i - 1 if i % 2 else i + 1) for i in range(slabs)]
    cross = lax.ppermute(to_cross, "slab", swap_cross)
    same = lax.ppermute(to_same, "slab", swap_same)
    blocks, trace, sources = call(
        combine_kernel,
        [("w", own), ("w", last), ("w", same), ("w", cross), ("w", meta), ("s", at)],
        [("w", (8 * slabs, LANES), F32), ("w", (8, LANES), F32), ("w", (256, 2 * per_list), BF16)],
    )
    traces = [trace]
    for k in range(1, groups):
        traces.append(lax.ppermute(trace, "probe", [(i, (i + k) % groups) for i in range(groups)]))
    (send,) = call(pack_kernel, [("w", blocks)] + [("w", x) for x in traces], [("w", (9 * slabs, LANES), F32)])
    got = lax.all_to_all(send.reshape(slabs, 1, 9 * LANES), "slab", 0, 0, tiled=True)
    (out,) = call(
        adjoint_kernel,
        [("w", sources), ("w", meta), ("s", flag)],
        [("h", fields.shape, BF16)],
        [pltpu.VMEM((16, tiles, 16, LANES), BF16), pltpu.SemaphoreType.DMA((OUT_CHUNKS, 4))],
    )
    count = probe_fields.shape[0] * groups * sensor_rows.shape[0]
    observed, total = call(
        finish_kernel,
        [("w", got.reshape(9 * slabs, LANES)), ("w", place)],
        [("v", (64, LANES), F32), ("v", (1, 1), F32)],
        scale=1.0 / count,
    )
    adjoint = out.transpose(0, 1, 3, 2, 4).reshape(probe_fields.shape)
    return adjoint, observed, total.reshape(())


def solution(mesh):
    placed = (P("probe", "slab", None), P(), P(), P(), P(), P(), P())

    return jax.shard_map(
        body,
        mesh=mesh,
        in_specs=placed,
        out_specs=(P("probe", "slab", None), P("probe", "slab"), P()),
        check_vma=False,
    )
```

```python
import functools

import jax
import jax.numpy as jnp
from jax import lax
from jax.experimental import pallas as pl
from jax.experimental.pallas import tpu as pltpu
from jax.sharding import PartitionSpec as P

F32 = jnp.float32
BF16 = jnp.bfloat16
LANES = 128
SLOTS = 16
VMEM_LIMIT = 32 * 2**20
CHUNKS = 2
OUT_CHUNKS = 8


def iota(shape, dim):
    return lax.broadcasted_iota(jnp.int32, shape, dim)


def one_hot(mask):
    return jnp.where(mask, 1.0, 0.0).astype(BF16)


def dot(a, b, dims=((1,), (0,))):
    return lax.dot_general(a, b, (dims, ((), ())), preferred_element_type=F32)


def pieces(x):
    high = x.astype(BF16)
    return high, (x - high.astype(F32)).astype(BF16)


def lookup_rows(order_hi, order_lo, rows):
    out = jnp.zeros(rows.shape, jnp.int32)
    for h in range(rows.shape[0]):
        line = jnp.broadcast_to(rows[h : h + 1, :], rows.shape)
        got = jnp.take_along_axis(line, order_lo, axis=1, mode="promise_in_bounds")
        out = jnp.where(order_hi == h, got, out)
    return out


def owner_slots(slab, owned_rows):
    upper = one_hot(iota((LANES, LANES), 0) < iota((LANES, LANES), 1))
    match = owned_rows // 4 == slab
    last = match & (owned_rows % 4 == 3)
    rank = dot(one_hot(match & ~last), upper)
    back_rank = dot(one_hot(last), upper)
    many = jnp.max(jnp.where(last & (back_rank > 7.5), 1.0, 0.0))
    return jnp.where(last, SLOTS - 1.0 - back_rank, jnp.where(match, rank, -1.0)).astype(BF16), many


def slot_fields(slab, slots, pieces_of, order_hi, order_lo, rows, cols, row_frac, col_frac, weights):
    owners = rows.shape[0]
    part = owners * 8
    lanes = iota((owners, part), 1)
    owner_of = one_hot((lanes // 8) % owners == iota((owners, part), 0))
    spread = [dot(x, owner_of, ((0,), (0,))) for x in slots]
    place = (iota((1, part), 1) % 8).astype(F32)
    pick = jnp.concatenate([jnp.where(spread[q] == place + 8.0 * half, 1.0, 0.0) for q, half in pieces_of], axis=1)
    present = jnp.sum(pick, axis=0, keepdims=True)
    total = pick.shape[1]
    owner_mask = jnp.concatenate([owner_of.astype(F32)] * len(pieces_of), axis=1)
    ids = jnp.concatenate([order_hi, order_lo], axis=0).astype(F32).astype(BF16)
    got = dot(ids, pick.astype(BF16))
    id_hi = jnp.sum(got[:owners] * owner_mask, axis=0, keepdims=True)
    id_lo = jnp.sum(got[owners:] * owner_mask, axis=0, keepdims=True)
    lo_iota = iota((LANES, total), 0).astype(F32)
    low_pick = jnp.where(lo_iota == id_lo, present, 0.0).astype(BF16)
    hi_mask = jnp.where(iota((owners, total), 0).astype(F32) == id_hi, 1.0, 0.0)
    table = [rows.astype(F32).astype(BF16), (cols // LANES).astype(F32).astype(BF16), (cols % LANES).astype(F32).astype(BF16)]
    table += list(pieces(row_frac))
    table += [(1.0 - col_frac).astype(BF16), col_frac.astype(BF16)]
    table += list(pieces(weights))
    got = dot(jnp.concatenate(table, axis=0), low_pick)
    field = [jnp.sum(got[owners * n : owners * (n + 1)] * hi_mask, axis=0, keepdims=True) for n in range(len(table))]
    row, tile, inner, frac, clow, chigh, weight = (
        field[0], field[1], field[2], field[3] + field[4], field[5], field[6], field[7] + field[8],
    )
    local = (slab * 4).astype(F32)
    sides = []
    for r in range(4):
        here = local + r
        sides.append(jnp.where(row == here, 1.0 - frac, jnp.where(row + 1.0 == here, frac, 0.0)))
    return jnp.concatenate([tile, inner, clow, chigh] + sides + [weight] + [jnp.zeros_like(tile)] * 7, axis=0)


def column_parts(meta):
    tile, inner, clow, chigh = (meta[n : n + 1] for n in range(4))
    count = inner.shape[1]
    cell = iota((LANES, count), 0).astype(F32)
    main = jnp.where(cell == inner, clow, jnp.where(cell == inner + 1.0, chigh, 0.0)).astype(BF16)
    first = iota((16, count), 0) == 0
    carry = jnp.where(first & (inner == LANES - 1.0), chigh, 0.0).astype(BF16)
    return main, carry, jnp.broadcast_to(tile, (16, count)).astype(BF16)


def row_sides(meta):
    return jnp.tile(jnp.concatenate([meta[4:8]] * 2, axis=0), (32, 1))


def column_table(number, tile, main, carry):
    one = jnp.ones((), BF16)
    zero = jnp.zeros((), BF16)
    first = 2.0 * number if isinstance(number, int) else 2.0 * number.astype(F32)
    is_tile = [jnp.where(tile == first + k, 1.0, 0.0).astype(BF16) if tile.dtype == F32 else jnp.where(tile == first + k, one, zero) for k in (-1, 0, 1)]
    parts = []
    for k in (0, 1):
        parts.append(main[:16] * is_tile[k + 1] + carry * is_tile[k])
        for g in range(1, 8):
            parts.append(main[16 * g : 16 * g + 16] * is_tile[k + 1])
    return jnp.concatenate(parts, axis=0)


def row_sum(x, group):
    count = x.shape[0] // group
    gather = one_hot(iota((count, x.shape[0]), 0) == iota((count, x.shape[0]), 1) // group)
    high, low = pieces(x)
    return dot(gather, high) + dot(gather, low)


def to_blocks(value):
    half = value.shape[1] // 2
    return jnp.concatenate([value[:, :half], value[:, half:]], axis=0).T


def field_block(scr, n):
    return jnp.concatenate([scr[:, 2 * n + m].reshape(256, LANES) for m in (0, 1)], axis=1)


def forward_kernel(
    slab_ref, rows_hbm, cols_hbm, rf_hbm, cf_hbm, w_hbm, order_hbm, u_ref,
    last_ref, same_ref, cross_ref, own_ref, meta_ref, place_ref, flag_ref, scr,
    small_i, small_f, sem, small_sem,
):
    chunks = CHUNKS
    width = scr.shape[1] // chunks

    def copy(c, k):
        where = pl.ds(c * width, width)
        return pltpu.make_async_copy(u_ref.at[:, k, where], scr.at[:, where, pl.ds(4 * k, 4)], sem.at[c, k])

    small = [
        pltpu.make_async_copy(src, dst, small_sem.at[n])
        for n, (src, dst) in enumerate(
            [(order_hbm, small_i.at[0]), (rows_hbm, small_i.at[1]), (cols_hbm, small_i.at[2])]
            + [(rf_hbm, small_f.at[0]), (cf_hbm, small_f.at[1]), (w_hbm, small_f.at[2])]
        )
    ]
    for x in small:
        x.start()
    for c in range(chunks):
        for k in range(4):
            copy(c, k).start()
    for x in small:
        x.wait()
    slab = slab_ref[0]
    order = small_i[0]
    order_hi = order // LANES
    order_lo = order % LANES
    rows = small_i[1]
    owned_rows = lookup_rows(order_hi, order_lo, rows)
    count = last_ref.shape[1]
    skip = count // 2
    given = (order_hi, order_lo, rows, small_i[2], small_f[0], small_f[1], small_f[2])
    own_slots, own_many = owner_slots(slab, owned_rows)
    last_slots, last_many = owner_slots(slab - 1, owned_rows)
    flag_ref[0] = (jnp.maximum(own_many, last_many) > 0.5).astype(jnp.int32)
    meta = slot_fields(slab, (own_slots, last_slots), ((0, 0), (0, 1), (1, 1)), *given)
    meta_ref[:, :count] = meta[:, :count]
    meta_ref[:, count : count + skip] = jnp.zeros((16, skip), F32)
    meta_ref[:, count + skip :] = meta[:, count:]
    own_rows = jnp.sum(jnp.where(iota(owned_rows.shape, 0) == slab, owned_rows, 0).astype(F32), axis=0, keepdims=True)
    own = jnp.floor(own_rows * 0.25)
    on_last = jnp.where(own_rows - own * 4.0 == 3.0, 1.0, 0.0)
    kind = jnp.broadcast_to(own * 2.0 + on_last, (LANES, LANES))
    before = (kind == kind.T) & (iota((LANES, LANES), 0) < iota((LANES, LANES), 1))
    rank = jnp.sum(jnp.where(before, 1.0, 0.0), axis=0, keepdims=True)
    rank = jnp.where(on_last > 0.5, SLOTS - 1.0 - rank, rank)
    half = jnp.where(rank >= 8.0, 1.0, 0.0)
    place_ref[...] = jnp.concatenate([own * 8.0 + rank - 8.0 * half, half] + [jnp.zeros_like(own)] * 6, axis=0)
    near = meta[:, skip:]
    main, carry, tile16 = column_parts(near)
    acc = jnp.zeros((256, count), F32)
    for c in range(chunks):
        for k in range(4):
            copy(c, k).wait()
        for n in range(c * width // 2, (c + 1) * width // 2):
            acc = acc + dot(field_block(scr, n), column_table(n, tile16, main, carry))
    part = row_sum(acc * row_sides(near), 4)
    even = slab % 2 == 0
    own_ref[...] = part[:, :skip]

    def give(own_first, last_first, part):
        own = jnp.concatenate([own_first, part[:, :skip]], axis=1)
        last = jnp.concatenate([last_first, part[:, skip:]], axis=1)
        last_ref[...] = last
        same_ref[...] = jnp.where(even, own, last)
        cross_ref[...] = jnp.where(even, last, own)

    nothing = jnp.zeros((64, skip), F32)
    give(nothing, nothing, part)

    @pl.when(flag_ref[0] != 0)
    def _():
        order = small_i[0]
        order_hi = order // LANES
        order_lo = order % LANES
        rows = small_i[1]
        slots, _ = owner_slots(slab - 1, lookup_rows(order_hi, order_lo, rows))
        given = (order_hi, order_lo, rows, small_i[2], small_f[0], small_f[1], small_f[2])
        meta_ref[:, count : count + skip] = slot_fields(slab, (slots,), ((0, 0),), *given)
        far = jnp.concatenate([meta_ref[:, :skip], meta_ref[:, count : count + skip]], axis=1)
        far_main, far_carry, _ = column_parts(far)
        far_tile = jnp.broadcast_to(far[:1], (16, count))

        def step(n, acc):
            return acc + dot(field_block(scr, n), column_table(n, far_tile, far_main, far_carry))

        acc = lax.fori_loop(0, scr.shape[1] // 2, step, jnp.zeros((256, count), F32))
        first = row_sum(acc * row_sides(far), 4)
        give(first[:, :skip], first[:, skip:], jnp.concatenate([own_ref[...], last_ref[:, skip:]], axis=1))


def rest_kernel(scr, meta_ref, part_ref):
    meta = meta_ref[:, : part_ref.shape[1]]
    main, carry, tile16 = column_parts(meta)
    sums = [jnp.zeros((128, part_ref.shape[1]), F32)] * 2
    for n in range(scr.shape[1] // 2):
        block = field_block(scr, n)
        table = column_table(n, tile16, main, carry)
        for m in (0, 1):
            sums[m] = sums[m] + dot(block[128 * m : 128 * m + 128], table)
    part_ref[...] = row_sum(jnp.concatenate(sums, axis=0) * row_sides(meta), 4)


def combine_kernel(rest_ref, own_ref, last_ref, same_ref, cross_ref, meta_ref, at_ref, block_ref, trace_ref, src_ref):
    count = last_ref.shape[1]
    even = at_ref[0] % 2 == 0
    own = jnp.concatenate([rest_ref[...], own_ref[...]], axis=1)
    same = same_ref[...]
    cross = cross_ref[...]
    value = own + jnp.where(even, same, cross)
    before = last_ref[...] + jnp.where(even, cross, same)
    weight = meta_ref[8:9, :]
    spread = jnp.concatenate([value, before], axis=1) * weight
    squares = jnp.sum(spread[:, :count] * value, axis=0, keepdims=True)
    trace = jnp.sum(squares, axis=1, keepdims=True)
    lines = to_blocks(value)
    block_ref[...] = lines
    trace_ref[...] = jnp.broadcast_to(trace, trace_ref.shape)
    repeat = one_hot(iota((256, 64), 0) // 4 == iota((256, 64), 1))
    tall = dot(repeat, spread.astype(BF16))
    src_ref[...] = (tall * row_sides(meta_ref[...])).astype(BF16)


def adjoint_kernel(src_ref, meta_ref, flag_ref, out_ref, scr, sem):
    chunks = OUT_CHUNKS
    width = scr.shape[1] // chunks

    def copy(c, k):
        return pltpu.make_async_copy(
            scr.at[:, pl.ds(c * width, width), pl.ds(4 * k, 4)], out_ref.at[:, k, pl.ds(c * width, width)], sem.at[c, k]
        )

    def spread_all(keep):
        main, carry, tile16 = column_parts(keep(meta_ref[...]))
        sources = keep(src_ref[...])
        for c in range(chunks):
            for n in range(c * width // 2, (c + 1) * width // 2):
                table = column_table(n, tile16, main, carry)
                cells = dot(sources, table, ((1,), (1,))).astype(BF16)
                scr[:, 2 * n] = cells[:, :LANES].reshape(16, 16, LANES)
                scr[:, 2 * n + 1] = cells[:, LANES:].reshape(16, 16, LANES)
            for k in range(4):
                copy(c, k).start()

    count = meta_ref.shape[1] // 2

    @pl.when(flag_ref[0] == 0)
    def _():
        spread_all(lambda x: jnp.concatenate([x[:, :count], x[:, count + count // 2 :]], axis=1))

    @pl.when(flag_ref[0] != 0)
    def _():
        spread_all(lambda x: x)

    for c in range(chunks):
        for k in range(4):
            copy(c, k).wait()


def pack_kernel(block_ref, *refs):
    *trace_refs, send_ref = refs
    trace = sum(ref[...] for ref in trace_refs)[:1, :]
    for o in range(block_ref.shape[0] // 8):
        send_ref[9 * o : 9 * o + 8, :] = block_ref[8 * o : 8 * o + 8, :]
        send_ref[9 * o + 8 : 9 * o + 9, :] = trace


def finish_kernel(got_ref, place_ref, observed_ref, total_ref, *, scale):
    slabs = got_ref.shape[0] // 9
    values = jnp.concatenate([got_ref[9 * q : 9 * q + 8, :] for q in range(slabs)], axis=0)
    pick = one_hot(iota((8 * slabs, LANES), 0).astype(F32) == place_ref[0:1, :])
    found = sum(dot(part, pick, ((0,), (0,))) for part in pieces(values))
    observed_ref[...] = jnp.where(place_ref[1:2, :] > 0.5, found[64:], found[:64])
    traces = jnp.sum(got_ref[pl.ds(8, slabs, stride=9), :], axis=0, keepdims=True)
    total_ref[...] = traces[:, :1] * scale


def call(kernel, inputs, outs, scratch=(), **params):
    kinds = {"v": pltpu.VMEM, "s": pltpu.SMEM, "h": pltpu.HBM, "w": pltpu.VMEM}
    held = {"w": pltpu.VMEM, "h": pltpu.HBM}
    arrays = [pltpu.with_memory_space_constraint(x, held[k]) if k in held else x for k, x in inputs]
    return pl.pallas_call(
        functools.partial(kernel, **params),
        in_specs=[pl.BlockSpec(memory_space=kinds[k]) for k, _ in inputs],
        out_specs=[pl.BlockSpec(memory_space=kinds[k]) for k, _, _ in outs],
        out_shape=[pltpu.VMEM(s, t) if k == "w" else jax.ShapeDtypeStruct(s, t) for k, s, t in outs],
        scratch_shapes=list(scratch),
        compiler_params=pltpu.CompilerParams(vmem_limit_bytes=VMEM_LIMIT),
    )(*arrays)


def body(probe_fields, sensor_rows, sensor_cols, row_frac, col_frac, sensor_weights, owner_order):
    at = lax.axis_index("slab").astype(jnp.int32).reshape(1)
    slabs = lax.axis_size("slab")
    groups = lax.axis_size("probe")
    per_list = slabs * SLOTS
    tiles = probe_fields.shape[2] // LANES
    fields = probe_fields.reshape(16, 4, 4, tiles, LANES).transpose(0, 1, 3, 2, 4)
    flat = [x.reshape(slabs, LANES) for x in (sensor_rows, sensor_cols, row_frac, col_frac, sensor_weights, owner_order)]
    half = per_list // 2
    last, to_same, to_cross, own, meta, place, flag, lines = call(
        forward_kernel,
        [("s", at)] + [("h", x) for x in flat] + [("h", fields)],
        [("w", (64, per_list), F32)] * 3
        + [("w", (64, half), F32), ("w", (16, 2 * per_list), F32), ("w", (8, LANES), F32), ("s", (1,), jnp.int32)]
        + [("w", (16, tiles, 16, LANES), BF16)],
        [
            pltpu.VMEM((3, slabs, LANES), jnp.int32),
            pltpu.VMEM((3, slabs, LANES), F32),
            pltpu.SemaphoreType.DMA((CHUNKS, 4)),
            pltpu.SemaphoreType.DMA((6,)),
        ],
    )
    swap_cross = [(i, i + 1 if i % 2 else i - 1) for i in range(1, slabs - 1)]
    swap_same = [(i, i - 1 if i % 2 else i + 1) for i in range(slabs)]
    cross = lax.ppermute(to_cross, "slab", swap_cross)
    same = lax.ppermute(to_same, "slab", swap_same)
    (rest,) = call(rest_kernel, [("w", lines), ("w", meta)], [("w", (64, half), F32)])
    blocks, trace, sources = call(
        combine_kernel,
        [("w", rest), ("w", own), ("w", last), ("w", same), ("w", cross), ("w", meta), ("s", at)],
        [("w", (8 * slabs, LANES), F32), ("w", (8, LANES), F32), ("w", (256, 2 * per_list), BF16)],
    )
    traces = [trace]
    for k in range(1, groups):
        traces.append(lax.ppermute(trace, "probe", [(i, (i + k) % groups) for i in range(groups)]))
    (send,) = call(pack_kernel, [("w", blocks)] + [("w", x) for x in traces], [("w", (9 * slabs, LANES), F32)])
    got = lax.all_to_all(send.reshape(slabs, 1, 9 * LANES), "slab", 0, 0, tiled=True)
    (out,) = call(
        adjoint_kernel,
        [("w", sources), ("w", meta), ("s", flag)],
        [("h", fields.shape, BF16)],
        [pltpu.VMEM((16, tiles, 16, LANES), BF16), pltpu.SemaphoreType.DMA((OUT_CHUNKS, 4))],
    )
    count = probe_fields.shape[0] * groups * sensor_rows.shape[0]
    observed, total = call(
        finish_kernel,
        [("w", got.reshape(9 * slabs, LANES)), ("w", place)],
        [("v", (64, LANES), F32), ("v", (1, 1), F32)],
        scale=1.0 / count,
    )
    adjoint = out.transpose(0, 1, 3, 2, 4).reshape(probe_fields.shape)
    return adjoint, observed, total.reshape(())


def solution(mesh):
    placed = (P("probe", "slab", None), P(), P(), P(), P(), P(), P())

    return jax.shard_map(
        body,
        mesh=mesh,
        in_specs=placed,
        out_specs=(P("probe", "slab", None), P("probe", "slab"), P()),
        check_vma=False,
    )
```

```python
import functools

import jax
import jax.numpy as jnp
from jax import lax
from jax.experimental import pallas as pl
from jax.experimental.pallas import tpu as pltpu
from jax.sharding import PartitionSpec as P

F32 = jnp.float32
BF16 = jnp.bfloat16
LANES = 128
SLOTS = 16
VMEM_LIMIT = 32 * 2**20
CHUNKS = 2
OUT_CHUNKS = 8


def iota(shape, dim):
    return lax.broadcasted_iota(jnp.int32, shape, dim)


def one_hot(mask):
    return jnp.where(mask, 1.0, 0.0).astype(BF16)


def dot(a, b, dims=((1,), (0,))):
    return lax.dot_general(a, b, (dims, ((), ())), preferred_element_type=F32)


def pieces(x):
    high = x.astype(BF16)
    return high, (x - high.astype(F32)).astype(BF16)


def lookup_rows(order_hi, order_lo, rows):
    out = jnp.zeros(rows.shape, jnp.int32)
    for h in range(rows.shape[0]):
        line = jnp.broadcast_to(rows[h : h + 1, :], rows.shape)
        got = jnp.take_along_axis(line, order_lo, axis=1, mode="promise_in_bounds")
        out = jnp.where(order_hi == h, got, out)
    return out


def owner_slots(slab, owned_rows):
    upper = one_hot(iota((LANES, LANES), 0) < iota((LANES, LANES), 1))
    match = owned_rows // 4 == slab
    last = match & (owned_rows % 4 == 3)
    rank = dot(one_hot(match & ~last), upper)
    back_rank = dot(one_hot(last), upper)
    many = jnp.max(jnp.where(last, back_rank + 1.0, 0.0))
    return jnp.where(last, SLOTS - 1.0 - back_rank, jnp.where(match, rank, -1.0)).astype(BF16), many


def slot_fields(slab, slots, pieces_of, order_hi, order_lo, rows, cols, row_frac, col_frac, weights):
    owners = rows.shape[0]
    part = owners * 4
    lanes = iota((owners, part), 1)
    owner_of = one_hot(lanes // 4 == iota((owners, part), 0))
    spread = [dot(x, owner_of, ((0,), (0,))) for x in slots]
    place = (iota((1, part), 1) % 4).astype(F32)
    pick = jnp.concatenate([jnp.where(spread[q] == place + 4.0 * quarter, 1.0, 0.0) for q, quarter in pieces_of], axis=1)
    present = jnp.sum(pick, axis=0, keepdims=True)
    total = pick.shape[1]
    owner_mask = jnp.concatenate([owner_of.astype(F32)] * len(pieces_of), axis=1)
    ids = jnp.concatenate([order_hi, order_lo], axis=0).astype(F32).astype(BF16)
    got = dot(ids, pick.astype(BF16))
    id_hi = jnp.sum(got[:owners] * owner_mask, axis=0, keepdims=True)
    id_lo = jnp.sum(got[owners:] * owner_mask, axis=0, keepdims=True)
    lo_iota = iota((LANES, total), 0).astype(F32)
    low_pick = jnp.where(lo_iota == id_lo, present, 0.0).astype(BF16)
    hi_mask = jnp.where(iota((owners, total), 0).astype(F32) == id_hi, 1.0, 0.0)
    table = [rows.astype(F32).astype(BF16), (cols // LANES).astype(F32).astype(BF16), (cols % LANES).astype(F32).astype(BF16)]
    table += list(pieces(row_frac))
    table += [(1.0 - col_frac).astype(BF16), col_frac.astype(BF16)]
    table += list(pieces(weights))
    got = dot(jnp.concatenate(table, axis=0), low_pick)
    field = [jnp.sum(got[owners * n : owners * (n + 1)] * hi_mask, axis=0, keepdims=True) for n in range(len(table))]
    row, tile, inner, frac, clow, chigh, weight = (
        field[0], field[1], field[2], field[3] + field[4], field[5], field[6], field[7] + field[8],
    )
    local = (slab * 4).astype(F32)
    sides = []
    for r in range(4):
        here = local + r
        sides.append(jnp.where(row == here, 1.0 - frac, jnp.where(row + 1.0 == here, frac, 0.0)))
    return jnp.concatenate([tile, inner, clow, chigh] + sides + [weight] + [jnp.zeros_like(tile)] * 7, axis=0)


def column_parts(meta):
    tile, inner, clow, chigh = (meta[n : n + 1] for n in range(4))
    count = inner.shape[1]
    cell = iota((LANES, count), 0).astype(F32)
    main = jnp.where(cell == inner, clow, jnp.where(cell == inner + 1.0, chigh, 0.0)).astype(BF16)
    first = iota((16, count), 0) == 0
    carry = jnp.where(first & (inner == LANES - 1.0), chigh, 0.0).astype(BF16)
    return main, carry, jnp.broadcast_to(tile, (16, count)).astype(BF16)


def row_sides(meta):
    return jnp.tile(jnp.concatenate([meta[4:8]] * 2, axis=0), (32, 1))


def column_table(number, tile, main, carry):
    one = jnp.ones((), BF16)
    zero = jnp.zeros((), BF16)
    is_tile = [jnp.where(tile == float(2 * number + k), one, zero) for k in (-1, 0, 1)]
    parts = []
    for k in (0, 1):
        parts.append(main[:16] * is_tile[k + 1] + carry * is_tile[k])
        for g in range(1, 8):
            parts.append(main[16 * g : 16 * g + 16] * is_tile[k + 1])
    return jnp.concatenate(parts, axis=0)


def row_sum(x, group):
    count = x.shape[0] // group
    gather = one_hot(iota((count, x.shape[0]), 0) == iota((count, x.shape[0]), 1) // group)
    high, low = pieces(x)
    return dot(gather, high) + dot(gather, low)


def field_block(scr, n):
    return jnp.concatenate([scr[:, 2 * n + m].reshape(256, LANES) for m in (0, 1)], axis=1)


def forward_kernel(
    slab_ref, rows_hbm, cols_hbm, rf_hbm, cf_hbm, w_hbm, order_hbm, u_ref,
    last_ref, same_ref, cross_ref, own_ref, meta_ref, place_ref, flag_ref, scr,
    small_i, small_f, sem, small_sem,
):
    chunks = CHUNKS
    width = scr.shape[1] // chunks

    def copy(c, k):
        where = pl.ds(c * width, width)
        return pltpu.make_async_copy(u_ref.at[:, k, where], scr.at[:, where, pl.ds(4 * k, 4)], sem.at[c, k])

    small = [
        pltpu.make_async_copy(src, dst, small_sem.at[n])
        for n, (src, dst) in enumerate(
            [(order_hbm, small_i.at[0]), (rows_hbm, small_i.at[1]), (cols_hbm, small_i.at[2])]
            + [(rf_hbm, small_f.at[0]), (cf_hbm, small_f.at[1]), (w_hbm, small_f.at[2])]
        )
    ]
    for x in small:
        x.start()
    for c in range(chunks):
        for k in range(4):
            copy(c, k).start()
    for x in small:
        x.wait()
    slab = slab_ref[0]
    order = small_i[0]
    order_hi = order // LANES
    order_lo = order % LANES
    rows = small_i[1]
    owned_rows = lookup_rows(order_hi, order_lo, rows)
    count = last_ref.shape[1]
    skip = count // 2
    given = (order_hi, order_lo, rows, small_i[2], small_f[0], small_f[1], small_f[2])
    own_slots, own_many = owner_slots(slab, owned_rows)
    last_slots, last_many = owner_slots(slab - 1, owned_rows)
    flag_ref[0] = (last_many > 8.0).astype(jnp.int32)
    flag_ref[1] = (jnp.maximum(own_many, last_many) > 8.0).astype(jnp.int32)
    flag_ref[2] = (jnp.maximum(own_many, last_many) > 12.0).astype(jnp.int32)
    quarters = [(q, n) for q in (0, 1) for n in range(4)]
    meta = slot_fields(slab, (own_slots, last_slots), quarters, *given)
    meta_ref[...] = meta
    own_rows = jnp.sum(jnp.where(iota(owned_rows.shape, 0) == slab, owned_rows, 0).astype(F32), axis=0, keepdims=True)
    own = jnp.floor(own_rows * 0.25)
    on_last = jnp.where(own_rows - own * 4.0 == 3.0, 1.0, 0.0)
    kind = jnp.broadcast_to(own * 2.0 + on_last, (LANES, LANES))
    before = (kind == kind.T) & (iota((LANES, LANES), 0) < iota((LANES, LANES), 1))
    rank = jnp.sum(jnp.where(before, 1.0, 0.0), axis=0, keepdims=True)
    rank = jnp.where(on_last > 0.5, SLOTS - 1.0 - rank, rank)
    quarter = jnp.floor(rank * 0.25)
    pair = jnp.floor(rank * 0.125)
    half = quarter - 2.0 * pair
    place_ref[...] = jnp.concatenate([own * 8.0 + pair * 4.0 + rank - 4.0 * quarter, half] + [jnp.zeros_like(own)] * 6, axis=0)
    near = jnp.concatenate([meta[:, skip:count], meta[:, count + skip :]], axis=1)
    main, carry, tile16 = column_parts(near)
    acc = jnp.zeros((256, count), F32)
    for c in range(chunks):
        for k in range(4):
            copy(c, k).wait()
        for n in range(c * width // 2, (c + 1) * width // 2):
            acc = acc + dot(field_block(scr, n), column_table(n, tile16, main, carry))
    part = row_sum(acc * row_sides(near), 4)
    even = slab % 2 == 0
    own_ref[...] = part[:, :skip]

    def give(own_first, last_first, part):
        own = jnp.concatenate([own_first, part[:, :skip]], axis=1)
        last = jnp.concatenate([last_first, part[:, skip:]], axis=1)
        last_ref[...] = last
        same_ref[...] = jnp.where(even, own, last)
        cross_ref[...] = jnp.where(even, last, own)

    nothing = jnp.zeros((64, skip), F32)
    give(nothing, nothing, part)

    for quarter in (1, 0):
        lanes = slice(LANES * quarter, LANES * quarter + LANES)

        @pl.when(flag_ref[2 - quarter] != 0)
        def _():
            far = jnp.concatenate([meta_ref[:, lanes], meta_ref[:, count + lanes.start : count + lanes.stop]], axis=1)
            first = shared_parts(scr, far)
            own, last = first[:, :LANES], first[:, LANES:]
            last_ref[:, lanes] = last
            same_ref[:, lanes] = jnp.where(even, own, last)
            cross_ref[:, lanes] = jnp.where(even, last, own)


def shared_parts(scr, meta):
    main, carry, tile16 = column_parts(meta)
    sums = [jnp.zeros((128, meta.shape[1]), F32)] * 2
    for n in range(scr.shape[1] // 2):
        block = field_block(scr, n)
        table = column_table(n, tile16, main, carry)
        for m in (0, 1):
            sums[m] = sums[m] + dot(block[128 * m : 128 * m + 128], table)
    return row_sum(jnp.concatenate(sums, axis=0) * row_sides(meta), 4)


def rest_kernel(scr, meta_ref, part_ref):
    part_ref[...] = shared_parts(scr, meta_ref[:, : part_ref.shape[1]])


def combine_kernel(rest_ref, own_ref, last_ref, same_ref, cross_ref, meta_ref, at_ref, block_ref, trace_ref, src_ref):
    count = last_ref.shape[1]
    even = at_ref[0] % 2 == 0
    own = jnp.concatenate([rest_ref[...], own_ref[...]], axis=1)
    same = same_ref[...]
    cross = cross_ref[...]
    value = own + jnp.where(even, same, cross)
    before = last_ref[...] + jnp.where(even, cross, same)
    weight = meta_ref[8:9, :]
    spread = jnp.concatenate([value, before], axis=1) * weight
    squares = jnp.sum(spread[:, :count] * value, axis=0, keepdims=True)
    trace = jnp.sum(squares, axis=1, keepdims=True)
    for pair in (0, 1):
        quarters = [value[:, LANES * n : LANES * n + LANES] for n in (2 * pair, 2 * pair + 1)]
        lines = jnp.concatenate(quarters, axis=0).T
        for o in range(LANES // 4):
            block_ref[8 * o + 4 * pair : 8 * o + 4 * pair + 4, :] = lines[4 * o : 4 * o + 4]
    trace_ref[...] = jnp.broadcast_to(trace, trace_ref.shape)
    repeat = one_hot(iota((256, 64), 0) // 4 == iota((256, 64), 1))
    tall = dot(repeat, spread.astype(BF16))
    src_ref[...] = (tall * row_sides(meta_ref[...])).astype(BF16)


def adjoint_kernel(src_ref, meta_ref, flag_ref, out_ref, scr, sem):
    chunks = OUT_CHUNKS
    width = scr.shape[1] // chunks

    def copy(c, k):
        return pltpu.make_async_copy(
            scr.at[:, pl.ds(c * width, width), pl.ds(4 * k, 4)], out_ref.at[:, k, pl.ds(c * width, width)], sem.at[c, k]
        )

    def spread_all(keep):
        main, carry, tile16 = column_parts(keep(meta_ref[...]))
        sources = keep(src_ref[...])
        for c in range(chunks):
            for n in range(c * width // 2, (c + 1) * width // 2):
                table = column_table(n, tile16, main, carry)
                cells = dot(sources, table, ((1,), (1,))).astype(BF16)
                scr[:, 2 * n] = cells[:, :LANES].reshape(16, 16, LANES)
                scr[:, 2 * n + 1] = cells[:, LANES:].reshape(16, 16, LANES)
            for k in range(4):
                copy(c, k).start()

    count = meta_ref.shape[1] // 2

    @pl.when(flag_ref[0] == 0)
    def _():
        spread_all(lambda x: jnp.concatenate([x[:, :count], x[:, count + count // 2 :]], axis=1))

    @pl.when(flag_ref[0] != 0)
    def _():
        spread_all(lambda x: x)

    for c in range(chunks):
        for k in range(4):
            copy(c, k).wait()


def pack_kernel(block_ref, *refs):
    *trace_refs, send_ref = refs
    trace = sum(ref[...] for ref in trace_refs)[:1, :]
    for o in range(block_ref.shape[0] // 8):
        send_ref[9 * o : 9 * o + 8, :] = block_ref[8 * o : 8 * o + 8, :]
        send_ref[9 * o + 8 : 9 * o + 9, :] = trace


def finish_kernel(got_ref, place_ref, observed_ref, total_ref, *, scale):
    slabs = got_ref.shape[0] // 9
    values = jnp.concatenate([got_ref[9 * q : 9 * q + 8, :] for q in range(slabs)], axis=0)
    pick = one_hot(iota((8 * slabs, LANES), 0).astype(F32) == place_ref[0:1, :])
    found = sum(dot(part, pick, ((0,), (0,))) for part in pieces(values))
    observed_ref[...] = jnp.where(place_ref[1:2, :] > 0.5, found[64:], found[:64])
    traces = jnp.sum(got_ref[pl.ds(8, slabs, stride=9), :], axis=0, keepdims=True)
    total_ref[...] = traces[:, :1] * scale


def call(kernel, inputs, outs, scratch=(), **params):
    kinds = {"v": pltpu.VMEM, "s": pltpu.SMEM, "h": pltpu.HBM, "w": pltpu.VMEM}
    held = {"w": pltpu.VMEM, "h": pltpu.HBM}
    arrays = [pltpu.with_memory_space_constraint(x, held[k]) if k in held else x for k, x in inputs]
    return pl.pallas_call(
        functools.partial(kernel, **params),
        in_specs=[pl.BlockSpec(memory_space=kinds[k]) for k, _ in inputs],
        out_specs=[pl.BlockSpec(memory_space=kinds[k]) for k, _, _ in outs],
        out_shape=[pltpu.VMEM(s, t) if k == "w" else jax.ShapeDtypeStruct(s, t) for k, s, t in outs],
        scratch_shapes=list(scratch),
        compiler_params=pltpu.CompilerParams(vmem_limit_bytes=VMEM_LIMIT),
    )(*arrays)


def body(probe_fields, sensor_rows, sensor_cols, row_frac, col_frac, sensor_weights, owner_order):
    at = lax.axis_index("slab").astype(jnp.int32).reshape(1)
    slabs = lax.axis_size("slab")
    groups = lax.axis_size("probe")
    per_list = slabs * SLOTS
    tiles = probe_fields.shape[2] // LANES
    fields = probe_fields.reshape(16, 4, 4, tiles, LANES).transpose(0, 1, 3, 2, 4)
    flat = [x.reshape(slabs, LANES) for x in (sensor_rows, sensor_cols, row_frac, col_frac, sensor_weights, owner_order)]
    half = per_list // 2
    last, to_same, to_cross, own, meta, place, flag, lines = call(
        forward_kernel,
        [("s", at)] + [("h", x) for x in flat] + [("h", fields)],
        [("w", (64, per_list), F32)] * 3
        + [("w", (64, half), F32), ("w", (16, 2 * per_list), F32), ("w", (8, LANES), F32), ("s", (3,), jnp.int32)]
        + [("w", (16, tiles, 16, LANES), BF16)],
        [
            pltpu.VMEM((3, slabs, LANES), jnp.int32),
            pltpu.VMEM((3, slabs, LANES), F32),
            pltpu.SemaphoreType.DMA((CHUNKS, 4)),
            pltpu.SemaphoreType.DMA((6,)),
        ],
    )
    swap_cross = [(i, i + 1 if i % 2 else i - 1) for i in range(1, slabs - 1)]
    swap_same = [(i, i - 1 if i % 2 else i + 1) for i in range(slabs)]
    cross = lax.ppermute(to_cross, "slab", swap_cross)
    same = lax.ppermute(to_same, "slab", swap_same)
    (rest,) = call(rest_kernel, [("w", lines), ("w", meta)], [("w", (64, half), F32)])
    blocks, trace, sources = call(
        combine_kernel,
        [("w", rest), ("w", own), ("w", last), ("w", same), ("w", cross), ("w", meta), ("s", at)],
        [("w", (8 * slabs, LANES), F32), ("w", (8, LANES), F32), ("w", (256, 2 * per_list), BF16)],
    )
    traces = [trace]
    for k in range(1, groups):
        traces.append(lax.ppermute(trace, "probe", [(i, (i + k) % groups) for i in range(groups)]))
    (send,) = call(pack_kernel, [("w", blocks)] + [("w", x) for x in traces], [("w", (9 * slabs, LANES), F32)])
    got = lax.all_to_all(send.reshape(slabs, 1, 9 * LANES), "slab", 0, 0, tiled=True)
    (out,) = call(
        adjoint_kernel,
        [("w", sources), ("w", meta), ("s", flag)],
        [("h", fields.shape, BF16)],
        [pltpu.VMEM((16, tiles, 16, LANES), BF16), pltpu.SemaphoreType.DMA((OUT_CHUNKS, 4))],
    )
    count = probe_fields.shape[0] * groups * sensor_rows.shape[0]
    observed, total = call(
        finish_kernel,
        [("w", got.reshape(9 * slabs, LANES)), ("w", place)],
        [("v", (64, LANES), F32), ("v", (1, 1), F32)],
        scale=1.0 / count,
    )
    adjoint = out.transpose(0, 1, 3, 2, 4).reshape(probe_fields.shape)
    return adjoint, observed, total.reshape(())


def solution(mesh):
    placed = (P("probe", "slab", None), P(), P(), P(), P(), P(), P())

    return jax.shard_map(
        body,
        mesh=mesh,
        in_specs=placed,
        out_specs=(P("probe", "slab", None), P("probe", "slab"), P()),
        check_vma=False,
    )
```

```python
import functools

import jax
import jax.numpy as jnp
from jax import lax
from jax.experimental import pallas as pl
from jax.experimental.pallas import tpu as pltpu
from jax.sharding import PartitionSpec as P

F32 = jnp.float32
BF16 = jnp.bfloat16
LANES = 128
SLOTS = 16
VMEM_LIMIT = 32 * 2**20
CHUNKS = 2
OUT_CHUNKS = 8


def exchange_order(slabs):
    return list(range(slabs // 2, slabs)) + list(range(slabs // 2))[::-1]


def iota(shape, dim):
    return lax.broadcasted_iota(jnp.int32, shape, dim)


def one_hot(mask):
    return jnp.where(mask, 1.0, 0.0).astype(BF16)


def dot(a, b, dims=((1,), (0,))):
    return lax.dot_general(a, b, (dims, ((), ())), preferred_element_type=F32)


def pieces(x):
    high = x.astype(BF16)
    return high, (x - high.astype(F32)).astype(BF16)


def lookup_rows(order_hi, order_lo, rows):
    out = jnp.zeros(rows.shape, jnp.int32)
    for h in range(rows.shape[0]):
        line = jnp.broadcast_to(rows[h : h + 1, :], rows.shape)
        got = jnp.take_along_axis(line, order_lo, axis=1, mode="promise_in_bounds")
        out = jnp.where(order_hi == h, got, out)
    return out


def owner_slots(slab, owned_rows):
    upper = one_hot(iota((LANES, LANES), 0) < iota((LANES, LANES), 1))
    match = owned_rows // 4 == slab
    last = match & (owned_rows % 4 == 3)
    rank = dot(one_hot(match & ~last), upper)
    back_rank = dot(one_hot(last), upper)
    many = jnp.max(jnp.where(last, back_rank + 1.0, 0.0))
    return jnp.where(last, SLOTS - 1.0 - back_rank, jnp.where(match, rank, -1.0)).astype(BF16), many


def slot_fields(slab, slots, pieces_of, order_hi, order_lo, rows, cols, row_frac, col_frac, weights):
    owners = rows.shape[0]
    part = owners * 4
    lanes = iota((owners, part), 1)
    owner_of = one_hot(lanes // 4 == iota((owners, part), 0))
    spread = [dot(x, owner_of, ((0,), (0,))) for x in slots]
    place = (iota((1, part), 1) % 4).astype(F32)
    pick = jnp.concatenate([jnp.where(spread[q] == place + 4.0 * quarter, 1.0, 0.0) for q, quarter in pieces_of], axis=1)
    present = jnp.sum(pick, axis=0, keepdims=True)
    total = pick.shape[1]
    owner_mask = jnp.concatenate([owner_of.astype(F32)] * len(pieces_of), axis=1)
    ids = jnp.concatenate([order_hi, order_lo], axis=0).astype(F32).astype(BF16)
    got = dot(ids, pick.astype(BF16))
    id_hi = jnp.sum(got[:owners] * owner_mask, axis=0, keepdims=True)
    id_lo = jnp.sum(got[owners:] * owner_mask, axis=0, keepdims=True)
    lo_iota = iota((LANES, total), 0).astype(F32)
    low_pick = jnp.where(lo_iota == id_lo, present, 0.0).astype(BF16)
    hi_mask = jnp.where(iota((owners, total), 0).astype(F32) == id_hi, 1.0, 0.0)
    table = [rows.astype(F32).astype(BF16), (cols // LANES).astype(F32).astype(BF16), (cols % LANES).astype(F32).astype(BF16)]
    table += list(pieces(row_frac))
    table += [(1.0 - col_frac).astype(BF16), col_frac.astype(BF16)]
    table += list(pieces(weights))
    got = dot(jnp.concatenate(table, axis=0), low_pick)
    field = [jnp.sum(got[owners * n : owners * (n + 1)] * hi_mask, axis=0, keepdims=True) for n in range(len(table))]
    row, tile, inner, frac, clow, chigh, weight = (
        field[0], field[1], field[2], field[3] + field[4], field[5], field[6], field[7] + field[8],
    )
    local = (slab * 4).astype(F32)
    sides = []
    for r in range(4):
        here = local + r
        sides.append(jnp.where(row == here, 1.0 - frac, jnp.where(row + 1.0 == here, frac, 0.0)))
    return jnp.concatenate([tile, inner, clow, chigh] + sides + [weight] + [jnp.zeros_like(tile)] * 7, axis=0)


def column_parts(meta):
    tile, inner, clow, chigh = (meta[n : n + 1] for n in range(4))
    count = inner.shape[1]
    cell = iota((LANES, count), 0).astype(F32)
    main = jnp.where(cell == inner, clow, jnp.where(cell == inner + 1.0, chigh, 0.0)).astype(BF16)
    first = iota((16, count), 0) == 0
    carry = jnp.where(first & (inner == LANES - 1.0), chigh, 0.0).astype(BF16)
    return main, carry, jnp.broadcast_to(tile, (16, count)).astype(BF16)


def row_sides(meta):
    return jnp.tile(jnp.concatenate([meta[4:8]] * 2, axis=0), (32, 1))


def column_table(number, tile, main, carry):
    one = jnp.ones((), BF16)
    zero = jnp.zeros((), BF16)
    is_tile = [jnp.where(tile == float(2 * number + k), one, zero) for k in (-1, 0, 1)]
    parts = []
    for k in (0, 1):
        parts.append(main[:16] * is_tile[k + 1] + carry * is_tile[k])
        for g in range(1, 8):
            parts.append(main[16 * g : 16 * g + 16] * is_tile[k + 1])
    return jnp.concatenate(parts, axis=0)


def row_sum(x, group):
    count = x.shape[0] // group
    gather = one_hot(iota((count, x.shape[0]), 0) == iota((count, x.shape[0]), 1) // group)
    high, low = pieces(x)
    return dot(gather, high) + dot(gather, low)


def field_block(scr, n):
    return jnp.concatenate([scr[:, 2 * n + m].reshape(256, LANES) for m in (0, 1)], axis=1)


def forward_kernel(
    slab_ref, rows_hbm, cols_hbm, rf_hbm, cf_hbm, w_hbm, order_hbm, u_ref,
    last_ref, same_ref, cross_ref, own_ref, meta_ref, place_ref, flag_ref, scr,
    small_i, small_f, sem, small_sem,
):
    chunks = CHUNKS
    width = scr.shape[1] // chunks

    def copy(c, k):
        where = pl.ds(c * width, width)
        return pltpu.make_async_copy(u_ref.at[:, k, where], scr.at[:, where, pl.ds(4 * k, 4)], sem.at[c, k])

    small = [
        pltpu.make_async_copy(src, dst, small_sem.at[n])
        for n, (src, dst) in enumerate(
            [(order_hbm, small_i.at[0]), (rows_hbm, small_i.at[1]), (cols_hbm, small_i.at[2])]
            + [(rf_hbm, small_f.at[0]), (cf_hbm, small_f.at[1]), (w_hbm, small_f.at[2])]
        )
    ]
    for x in small:
        x.start()
    for c in range(chunks):
        for k in range(4):
            copy(c, k).start()
    for x in small:
        x.wait()
    slab = slab_ref[0]
    order = small_i[0]
    order_hi = order // LANES
    order_lo = order % LANES
    rows = small_i[1]
    owned_rows = lookup_rows(order_hi, order_lo, rows)
    count = last_ref.shape[1]
    skip = count // 2
    given = (order_hi, order_lo, rows, small_i[2], small_f[0], small_f[1], small_f[2])
    own_slots, own_many = owner_slots(slab, owned_rows)
    last_slots, last_many = owner_slots(slab - 1, owned_rows)
    flag_ref[0] = (last_many > 8.0).astype(jnp.int32)
    flag_ref[1] = (jnp.maximum(own_many, last_many) > 8.0).astype(jnp.int32)
    flag_ref[2] = (jnp.maximum(own_many, last_many) > 12.0).astype(jnp.int32)
    quarters = [(q, n) for q in (0, 1) for n in range(4)]
    meta = slot_fields(slab, (own_slots, last_slots), quarters, *given)
    meta_ref[...] = meta
    own_rows = jnp.sum(jnp.where(iota(owned_rows.shape, 0) == slab, owned_rows, 0).astype(F32), axis=0, keepdims=True)
    own = jnp.floor(own_rows * 0.25)
    on_last = jnp.where(own_rows - own * 4.0 == 3.0, 1.0, 0.0)
    kind = jnp.broadcast_to(own * 2.0 + on_last, (LANES, LANES))
    before = (kind == kind.T) & (iota((LANES, LANES), 0) < iota((LANES, LANES), 1))
    rank = jnp.sum(jnp.where(before, 1.0, 0.0), axis=0, keepdims=True)
    rank = jnp.where(on_last > 0.5, SLOTS - 1.0 - rank, rank)
    quarter = jnp.floor(rank * 0.25)
    pair = jnp.floor(rank * 0.125)
    half = quarter - 2.0 * pair
    place_ref[...] = jnp.concatenate([own * 8.0 + pair * 4.0 + rank - 4.0 * quarter, half] + [jnp.zeros_like(own)] * 6, axis=0)
    near = jnp.concatenate([meta[:, skip:count], meta[:, count + skip :]], axis=1)
    main, carry, tile16 = column_parts(near)
    acc = jnp.zeros((256, count), F32)
    for c in range(chunks):
        for k in range(4):
            copy(c, k).wait()
        for n in range(c * width // 2, (c + 1) * width // 2):
            acc = acc + dot(field_block(scr, n), column_table(n, tile16, main, carry))
    part = row_sum(acc * row_sides(near), 4)
    even = slab % 2 == 0
    own_ref[...] = part[:, :skip]

    def give(own_first, last_first, part):
        own = jnp.concatenate([own_first, part[:, :skip]], axis=1)
        last = jnp.concatenate([last_first, part[:, skip:]], axis=1)
        last_ref[...] = last
        same_ref[...] = jnp.where(even, own, last)
        cross_ref[...] = jnp.where(even, last, own)

    nothing = jnp.zeros((64, skip), F32)
    give(nothing, nothing, part)

    for quarter in (1, 0):
        lanes = slice(LANES * quarter, LANES * quarter + LANES)

        @pl.when(flag_ref[2 - quarter] != 0)
        def _():
            far = jnp.concatenate([meta_ref[:, lanes], meta_ref[:, count + lanes.start : count + lanes.stop]], axis=1)
            first = shared_parts(scr, far)
            own, last = first[:, :LANES], first[:, LANES:]
            last_ref[:, lanes] = last
            same_ref[:, lanes] = jnp.where(even, own, last)
            cross_ref[:, lanes] = jnp.where(even, last, own)


def shared_parts(scr, meta):
    main, carry, tile16 = column_parts(meta)
    sums = [jnp.zeros((128, meta.shape[1]), F32)] * 2
    for n in range(scr.shape[1] // 2):
        block = field_block(scr, n)
        table = column_table(n, tile16, main, carry)
        for m in (0, 1):
            sums[m] = sums[m] + dot(block[128 * m : 128 * m + 128], table)
    return row_sum(jnp.concatenate(sums, axis=0) * row_sides(meta), 4)


def rest_kernel(scr, meta_ref, part_ref):
    part_ref[...] = shared_parts(scr, meta_ref[:, : part_ref.shape[1]])


def combine_kernel(rest_ref, own_ref, last_ref, same_ref, cross_ref, meta_ref, at_ref, block_ref, trace_ref, src_ref):
    count = last_ref.shape[1]
    even = at_ref[0] % 2 == 0
    own = jnp.concatenate([rest_ref[...], own_ref[...]], axis=1)
    same = same_ref[...]
    cross = cross_ref[...]
    value = own + jnp.where(even, same, cross)
    before = last_ref[...] + jnp.where(even, cross, same)
    weight = meta_ref[8:9, :]
    spread = jnp.concatenate([value, before], axis=1) * weight
    squares = jnp.sum(spread[:, :count] * value, axis=0, keepdims=True)
    trace = jnp.sum(squares, axis=1, keepdims=True)
    for pair in (0, 1):
        quarters = [value[:, LANES * n : LANES * n + LANES] for n in (2 * pair, 2 * pair + 1)]
        lines = jnp.concatenate(quarters, axis=0).T
        for o in range(LANES // 4):
            block_ref[8 * o + 4 * pair : 8 * o + 4 * pair + 4, :] = lines[4 * o : 4 * o + 4]
    trace_ref[...] = jnp.broadcast_to(trace, trace_ref.shape)
    repeat = one_hot(iota((256, 64), 0) // 4 == iota((256, 64), 1))
    tall = dot(repeat, spread.astype(BF16))
    src_ref[...] = (tall * row_sides(meta_ref[...])).astype(BF16)


def adjoint_kernel(src_ref, meta_ref, flag_ref, out_ref, scr, sem):
    chunks = OUT_CHUNKS
    width = scr.shape[1] // chunks

    def copy(c, k):
        return pltpu.make_async_copy(
            scr.at[:, pl.ds(c * width, width), pl.ds(4 * k, 4)], out_ref.at[:, k, pl.ds(c * width, width)], sem.at[c, k]
        )

    def spread_all(keep):
        main, carry, tile16 = column_parts(keep(meta_ref[...]))
        sources = keep(src_ref[...])
        for c in range(chunks):
            for n in range(c * width // 2, (c + 1) * width // 2):
                table = column_table(n, tile16, main, carry)
                cells = dot(sources, table, ((1,), (1,))).astype(BF16)
                scr[:, 2 * n] = cells[:, :LANES].reshape(16, 16, LANES)
                scr[:, 2 * n + 1] = cells[:, LANES:].reshape(16, 16, LANES)
            for k in range(4):
                copy(c, k).start()

    count = meta_ref.shape[1] // 2

    @pl.when(flag_ref[0] == 0)
    def _():
        spread_all(lambda x: jnp.concatenate([x[:, :count], x[:, count + count // 2 :]], axis=1))

    @pl.when(flag_ref[0] != 0)
    def _():
        spread_all(lambda x: x)

    for c in range(chunks):
        for k in range(4):
            copy(c, k).wait()


def pack_kernel(block_ref, *refs):
    *trace_refs, send_ref = refs
    trace = sum(ref[...] for ref in trace_refs)[:1, :]
    for n, o in enumerate(exchange_order(block_ref.shape[0] // 8)):
        send_ref[9 * n : 9 * n + 8, :] = block_ref[8 * o : 8 * o + 8, :]
        send_ref[9 * n + 8 : 9 * n + 9, :] = trace


def finish_kernel(got_ref, place_ref, observed_ref, total_ref, *, scale):
    slabs = got_ref.shape[0] // 9
    blocks = {q: got_ref[9 * n : 9 * n + 8, :] for n, q in enumerate(exchange_order(slabs))}
    values = jnp.concatenate([blocks[q] for q in range(slabs)], axis=0)
    pick = one_hot(iota((8 * slabs, LANES), 0).astype(F32) == place_ref[0:1, :])
    found = sum(dot(part, pick, ((0,), (0,))) for part in pieces(values))
    observed_ref[...] = jnp.where(place_ref[1:2, :] > 0.5, found[64:], found[:64])
    traces = jnp.sum(got_ref[pl.ds(8, slabs, stride=9), :], axis=0, keepdims=True)
    total_ref[...] = traces[:, :1] * scale


def call(kernel, inputs, outs, scratch=(), **params):
    kinds = {"v": pltpu.VMEM, "s": pltpu.SMEM, "h": pltpu.HBM, "w": pltpu.VMEM}
    held = {"w": pltpu.VMEM, "h": pltpu.HBM}
    arrays = [pltpu.with_memory_space_constraint(x, held[k]) if k in held else x for k, x in inputs]
    return pl.pallas_call(
        functools.partial(kernel, **params),
        in_specs=[pl.BlockSpec(memory_space=kinds[k]) for k, _ in inputs],
        out_specs=[pl.BlockSpec(memory_space=kinds[k]) for k, _, _ in outs],
        out_shape=[pltpu.VMEM(s, t) if k == "w" else jax.ShapeDtypeStruct(s, t) for k, s, t in outs],
        scratch_shapes=list(scratch),
        compiler_params=pltpu.CompilerParams(vmem_limit_bytes=VMEM_LIMIT),
    )(*arrays)


def body(probe_fields, sensor_rows, sensor_cols, row_frac, col_frac, sensor_weights, owner_order):
    at = lax.axis_index("slab").astype(jnp.int32).reshape(1)
    slabs = lax.axis_size("slab")
    groups = lax.axis_size("probe")
    per_list = slabs * SLOTS
    tiles = probe_fields.shape[2] // LANES
    fields = probe_fields.reshape(16, 4, 4, tiles, LANES).transpose(0, 1, 3, 2, 4)
    flat = [x.reshape(slabs, LANES) for x in (sensor_rows, sensor_cols, row_frac, col_frac, sensor_weights, owner_order)]
    half = per_list // 2
    last, to_same, to_cross, own, meta, place, flag, lines = call(
        forward_kernel,
        [("s", at)] + [("h", x) for x in flat] + [("h", fields)],
        [("w", (64, per_list), F32)] * 3
        + [("w", (64, half), F32), ("w", (16, 2 * per_list), F32), ("w", (8, LANES), F32), ("s", (3,), jnp.int32)]
        + [("w", (16, tiles, 16, LANES), BF16)],
        [
            pltpu.VMEM((3, slabs, LANES), jnp.int32),
            pltpu.VMEM((3, slabs, LANES), F32),
            pltpu.SemaphoreType.DMA((CHUNKS, 4)),
            pltpu.SemaphoreType.DMA((6,)),
        ],
    )
    swap_cross = [(i, i + 1 if i % 2 else i - 1) for i in range(1, slabs - 1)]
    swap_same = [(i, i - 1 if i % 2 else i + 1) for i in range(slabs)]
    cross = lax.ppermute(to_cross, "slab", swap_cross)
    same = lax.ppermute(to_same, "slab", swap_same)
    (rest,) = call(rest_kernel, [("w", lines), ("w", meta)], [("w", (64, half), F32)])
    blocks, trace, sources = call(
        combine_kernel,
        [("w", rest), ("w", own), ("w", last), ("w", same), ("w", cross), ("w", meta), ("s", at)],
        [("w", (8 * slabs, LANES), F32), ("w", (8, LANES), F32), ("w", (256, 2 * per_list), BF16)],
    )
    traces = [trace]
    for k in range(1, groups):
        traces.append(lax.ppermute(trace, "probe", [(i, (i + k) % groups) for i in range(groups)]))
    (send,) = call(pack_kernel, [("w", blocks)] + [("w", x) for x in traces], [("w", (9 * slabs, LANES), F32)])
    got = lax.all_to_all(
        send.reshape(slabs, 1, 9 * LANES), "slab", 0, 0, axis_index_groups=[exchange_order(slabs)], tiled=True
    )
    (out,) = call(
        adjoint_kernel,
        [("w", sources), ("w", meta), ("s", flag)],
        [("h", fields.shape, BF16)],
        [pltpu.VMEM((16, tiles, 16, LANES), BF16), pltpu.SemaphoreType.DMA((OUT_CHUNKS, 4))],
    )
    count = probe_fields.shape[0] * groups * sensor_rows.shape[0]
    observed, total = call(
        finish_kernel,
        [("w", got.reshape(9 * slabs, LANES)), ("w", place)],
        [("v", (64, LANES), F32), ("v", (1, 1), F32)],
        scale=1.0 / count,
    )
    adjoint = out.transpose(0, 1, 3, 2, 4).reshape(probe_fields.shape)
    return adjoint, observed, total.reshape(())


def solution(mesh):
    placed = (P("probe", "slab", None), P(), P(), P(), P(), P(), P())

    return jax.shard_map(
        body,
        mesh=mesh,
        in_specs=placed,
        out_specs=(P("probe", "slab", None), P("probe", "slab"), P()),
        check_vma=False,
    )
```

```python
import functools

import jax
import jax.numpy as jnp
from jax import lax
from jax.experimental import pallas as pl
from jax.experimental.pallas import tpu as pltpu
from jax.sharding import PartitionSpec as P

F32 = jnp.float32
BF16 = jnp.bfloat16
LANES = 128
SLOTS = 16
VMEM_LIMIT = 32 * 2**20
CHUNKS = 2
OUT_CHUNKS = 8


def exchange_order(slabs):
    return list(range(slabs // 2, slabs)) + list(range(slabs // 2))[::-1]


def iota(shape, dim):
    return lax.broadcasted_iota(jnp.int32, shape, dim)


def one_hot(mask):
    return jnp.where(mask, 1.0, 0.0).astype(BF16)


def dot(a, b, dims=((1,), (0,))):
    return lax.dot_general(a, b, (dims, ((), ())), preferred_element_type=F32)


def pieces(x):
    high = x.astype(BF16)
    return high, (x - high.astype(F32)).astype(BF16)


def lookup_rows(order_hi, order_lo, rows):
    out = jnp.zeros(rows.shape, jnp.int32)
    for h in range(rows.shape[0]):
        line = jnp.broadcast_to(rows[h : h + 1, :], rows.shape)
        got = jnp.take_along_axis(line, order_lo, axis=1, mode="promise_in_bounds")
        out = jnp.where(order_hi == h, got, out)
    return out


def owner_slots(slab, owned_rows):
    upper = one_hot(iota((LANES, LANES), 0) < iota((LANES, LANES), 1))
    match = owned_rows // 4 == slab
    last = match & (owned_rows % 4 == 3)
    rank = dot(one_hot(match & ~last), upper)
    back_rank = dot(one_hot(last), upper)
    many = jnp.max(jnp.where(last, back_rank + 1.0, 0.0))
    return jnp.where(last, SLOTS - 1.0 - back_rank, jnp.where(match, rank, -1.0)).astype(BF16), many


def slot_fields(slab, slots, pieces_of, order_hi, order_lo, rows, cols, row_frac, col_frac, weights):
    owners = rows.shape[0]
    part = owners * 4
    lanes = iota((owners, part), 1)
    owner_of = one_hot(lanes // 4 == iota((owners, part), 0))
    spread = [dot(x, owner_of, ((0,), (0,))) for x in slots]
    place = (iota((1, part), 1) % 4).astype(F32)
    pick = jnp.concatenate([jnp.where(spread[q] == place + 4.0 * quarter, 1.0, 0.0) for q, quarter in pieces_of], axis=1)
    present = jnp.sum(pick, axis=0, keepdims=True)
    total = pick.shape[1]
    owner_mask = jnp.concatenate([owner_of.astype(F32)] * len(pieces_of), axis=1)
    ids = jnp.concatenate([order_hi, order_lo], axis=0).astype(F32).astype(BF16)
    got = dot(ids, pick.astype(BF16))
    id_hi = jnp.sum(got[:owners] * owner_mask, axis=0, keepdims=True)
    id_lo = jnp.sum(got[owners:] * owner_mask, axis=0, keepdims=True)
    lo_iota = iota((LANES, total), 0).astype(F32)
    low_pick = jnp.where(lo_iota == id_lo, present, 0.0).astype(BF16)
    hi_mask = jnp.where(iota((owners, total), 0).astype(F32) == id_hi, 1.0, 0.0)
    table = [rows.astype(F32).astype(BF16), (cols // LANES).astype(F32).astype(BF16), (cols % LANES).astype(F32).astype(BF16)]
    table += list(pieces(row_frac))
    table += [(1.0 - col_frac).astype(BF16), col_frac.astype(BF16)]
    table += list(pieces(weights))
    got = dot(jnp.concatenate(table, axis=0), low_pick)
    field = [jnp.sum(got[owners * n : owners * (n + 1)] * hi_mask, axis=0, keepdims=True) for n in range(len(table))]
    row, tile, inner, frac, clow, chigh, weight = (
        field[0], field[1], field[2], field[3] + field[4], field[5], field[6], field[7] + field[8],
    )
    local = (slab * 4).astype(F32)
    sides = []
    for r in range(4):
        here = local + r
        sides.append(jnp.where(row == here, 1.0 - frac, jnp.where(row + 1.0 == here, frac, 0.0)))
    return jnp.concatenate([tile, inner, clow, chigh] + sides + [weight] + [jnp.zeros_like(tile)] * 7, axis=0)


def column_parts(meta):
    tile, inner, clow, chigh = (meta[n : n + 1] for n in range(4))
    count = inner.shape[1]
    cell = iota((LANES, count), 0).astype(F32)
    main = jnp.where(cell == inner, clow, jnp.where(cell == inner + 1.0, chigh, 0.0)).astype(BF16)
    first = iota((16, count), 0) == 0
    carry = jnp.where(first & (inner == LANES - 1.0), chigh, 0.0).astype(BF16)
    return main, carry, jnp.broadcast_to(tile, (16, count)).astype(BF16)


def row_sides(meta):
    return jnp.tile(jnp.concatenate([meta[4:8]] * 2, axis=0), (32, 1))


def column_table(number, tile, main, carry):
    one = jnp.ones((), BF16)
    zero = jnp.zeros((), BF16)
    is_tile = [jnp.where(tile == float(2 * number + k), one, zero) for k in (-1, 0, 1)]
    parts = []
    for k in (0, 1):
        parts.append(main[:16] * is_tile[k + 1] + carry * is_tile[k])
        for g in range(1, 8):
            parts.append(main[16 * g : 16 * g + 16] * is_tile[k + 1])
    return jnp.concatenate(parts, axis=0)


def row_sum(x, group):
    count = x.shape[0] // group
    gather = one_hot(iota((count, x.shape[0]), 0) == iota((count, x.shape[0]), 1) // group)
    high, low = pieces(x)
    return dot(gather, high) + dot(gather, low)


def field_block(scr, n):
    return jnp.concatenate([scr[:, 2 * n + m].reshape(256, LANES) for m in (0, 1)], axis=1)


def forward_kernel(
    slab_ref, rows_hbm, cols_hbm, rf_hbm, cf_hbm, w_hbm, order_hbm, u_ref,
    cross_ref, meta_ref, place_ref, flag_ref, scr,
    small_i, small_f, sem, small_sem,
):
    chunks = CHUNKS
    width = scr.shape[1] // chunks

    def copy(c, k):
        where = pl.ds(c * width, width)
        return pltpu.make_async_copy(u_ref.at[:, k, where], scr.at[:, where, pl.ds(4 * k, 4)], sem.at[c, k])

    small = [
        pltpu.make_async_copy(src, dst, small_sem.at[n])
        for n, (src, dst) in enumerate(
            [(order_hbm, small_i.at[0]), (rows_hbm, small_i.at[1]), (cols_hbm, small_i.at[2])]
            + [(rf_hbm, small_f.at[0]), (cf_hbm, small_f.at[1]), (w_hbm, small_f.at[2])]
        )
    ]
    for x in small:
        x.start()
    for c in range(chunks):
        for k in range(4):
            copy(c, k).start()
    for x in small:
        x.wait()
    slab = slab_ref[0]
    order = small_i[0]
    order_hi = order // LANES
    order_lo = order % LANES
    rows = small_i[1]
    owned_rows = lookup_rows(order_hi, order_lo, rows)
    count = cross_ref.shape[1]
    skip = count // 2
    given = (order_hi, order_lo, rows, small_i[2], small_f[0], small_f[1], small_f[2])
    own_slots, own_many = owner_slots(slab, owned_rows)
    last_slots, last_many = owner_slots(slab - 1, owned_rows)
    flag_ref[0] = (last_many > 8.0).astype(jnp.int32)
    flag_ref[1] = (jnp.maximum(own_many, last_many) > 8.0).astype(jnp.int32)
    flag_ref[2] = (jnp.maximum(own_many, last_many) > 12.0).astype(jnp.int32)
    flag_ref[3] = slab % 2
    quarters = [(q, n) for q in (0, 1) for n in range(4)]
    meta = slot_fields(slab, (own_slots, last_slots), quarters, *given)
    meta_ref[...] = meta
    own_rows = jnp.sum(jnp.where(iota(owned_rows.shape, 0) == slab, owned_rows, 0).astype(F32), axis=0, keepdims=True)
    own = jnp.floor(own_rows * 0.25)
    on_last = jnp.where(own_rows - own * 4.0 == 3.0, 1.0, 0.0)
    kind = jnp.broadcast_to(own * 2.0 + on_last, (LANES, LANES))
    before = (kind == kind.T) & (iota((LANES, LANES), 0) < iota((LANES, LANES), 1))
    rank = jnp.sum(jnp.where(before, 1.0, 0.0), axis=0, keepdims=True)
    rank = jnp.where(on_last > 0.5, SLOTS - 1.0 - rank, rank)
    quarter = jnp.floor(rank * 0.25)
    pair = jnp.floor(rank * 0.125)
    half = quarter - 2.0 * pair
    place_ref[...] = jnp.concatenate([own * 8.0 + pair * 4.0 + rank - 4.0 * quarter, half] + [jnp.zeros_like(own)] * 6, axis=0)
    near = jnp.where(slab % 2 == 0, meta[:, count + skip :], meta[:, skip:count])
    for k in range(4 * chunks):
        copy(k // 4, k % 4).wait()
    cross_ref[:, :skip] = jnp.zeros((64, skip), F32)
    cross_ref[:, skip:] = shared_parts(scr, near)
    far_parts(scr, meta_ref, flag_ref, cross_ref, 0)


def far_parts(scr, meta_ref, flag_ref, part_ref, parity):
    count = part_ref.shape[1]
    for quarter in (1, 0):
        lanes = slice(LANES * quarter, LANES * quarter + LANES)

        @pl.when(flag_ref[2 - quarter] != 0)
        def _():
            own, last = meta_ref[:, lanes], meta_ref[:, count + lanes.start : count + lanes.stop]
            part_ref[:, lanes] = shared_parts(scr, jnp.where(flag_ref[3] == parity, last, own))


def shared_parts(scr, meta):
    main, carry, tile16 = column_parts(meta)
    sums = [jnp.zeros((128, meta.shape[1]), F32)] * 2
    for n in range(scr.shape[1] // 2):
        block = field_block(scr, n)
        table = column_table(n, tile16, main, carry)
        for m in (0, 1):
            sums[m] = sums[m] + dot(block[128 * m : 128 * m + 128], table)
    return row_sum(jnp.concatenate(sums, axis=0) * row_sides(meta), 4)


def rest_kernel(scr, meta_ref, flag_ref, same_ref, part_ref):
    count = same_ref.shape[1]
    skip = count // 2
    near = jnp.where(flag_ref[3] == 1, meta_ref[:, count + skip :], meta_ref[:, skip:count])
    meta = jnp.concatenate([near, meta_ref[:, :skip]], axis=1)
    main, carry, tile16 = column_parts(meta)
    acc = jnp.zeros((256, count), F32)
    for n in range(scr.shape[1] // 2):
        acc = acc + dot(field_block(scr, n), column_table(n, tile16, main, carry))
    part = row_sum(acc * row_sides(meta), 4)
    part_ref[...] = part[:, skip:]
    same_ref[:, :skip] = jnp.zeros((64, skip), F32)
    same_ref[:, skip:] = part[:, :skip]
    far_parts(scr, meta_ref, flag_ref, same_ref, 1)


def combine_kernel(rest_ref, to_same_ref, to_cross_ref, same_ref, cross_ref, meta_ref, at_ref, block_ref, trace_ref, src_ref):
    count = same_ref.shape[1]
    even = at_ref[0] % 2 == 0
    same = same_ref[...]
    cross = cross_ref[...]
    to_same = to_same_ref[...]
    to_cross = to_cross_ref[...]
    own = jnp.concatenate([rest_ref[...], jnp.where(even, to_same, to_cross)[:, count // 2 :]], axis=1)
    value = own + jnp.where(even, same, cross)
    before = jnp.where(even, to_cross + cross, to_same + same)
    weight = meta_ref[8:9, :]
    spread = jnp.concatenate([value, before], axis=1) * weight
    squares = jnp.sum(spread[:, :count] * value, axis=0, keepdims=True)
    trace = jnp.sum(squares, axis=1, keepdims=True)
    for pair in (0, 1):
        quarters = [value[:, LANES * n : LANES * n + LANES] for n in (2 * pair, 2 * pair + 1)]
        lines = jnp.concatenate(quarters, axis=0).T
        for o in range(LANES // 4):
            block_ref[8 * o + 4 * pair : 8 * o + 4 * pair + 4, :] = lines[4 * o : 4 * o + 4]
    trace_ref[...] = jnp.broadcast_to(trace, trace_ref.shape)
    repeat = one_hot(iota((256, 64), 0) // 4 == iota((256, 64), 1))
    tall = dot(repeat, spread.astype(BF16))
    src_ref[...] = (tall * row_sides(meta_ref[...])).astype(BF16)


def adjoint_kernel(src_ref, meta_ref, flag_ref, out_ref, scr, sem):
    chunks = OUT_CHUNKS
    width = scr.shape[1] // chunks

    def copy(c, k):
        return pltpu.make_async_copy(
            scr.at[:, pl.ds(c * width, width), pl.ds(4 * k, 4)], out_ref.at[:, k, pl.ds(c * width, width)], sem.at[c, k]
        )

    def spread_all(keep):
        main, carry, tile16 = column_parts(keep(meta_ref[...]))
        sources = keep(src_ref[...])
        for c in range(chunks):
            for n in range(c * width // 2, (c + 1) * width // 2):
                table = column_table(n, tile16, main, carry)
                cells = dot(sources, table, ((1,), (1,))).astype(BF16)
                scr[:, 2 * n] = cells[:, :LANES].reshape(16, 16, LANES)
                scr[:, 2 * n + 1] = cells[:, LANES:].reshape(16, 16, LANES)
            for k in range(4):
                copy(c, k).start()

    count = meta_ref.shape[1] // 2

    @pl.when(flag_ref[0] == 0)
    def _():
        spread_all(lambda x: jnp.concatenate([x[:, :count], x[:, count + count // 2 :]], axis=1))

    @pl.when(flag_ref[0] != 0)
    def _():
        spread_all(lambda x: x)

    for c in range(chunks):
        for k in range(4):
            copy(c, k).wait()


def pack_kernel(block_ref, *refs):
    *trace_refs, send_ref = refs
    trace = sum(ref[...] for ref in trace_refs)[:1, :]
    for n, o in enumerate(exchange_order(block_ref.shape[0] // 8)):
        send_ref[9 * n : 9 * n + 8, :] = block_ref[8 * o : 8 * o + 8, :]
        send_ref[9 * n + 8 : 9 * n + 9, :] = trace


def finish_kernel(got_ref, place_ref, observed_ref, total_ref, *, scale):
    slabs = got_ref.shape[0] // 9
    blocks = {q: got_ref[9 * n : 9 * n + 8, :] for n, q in enumerate(exchange_order(slabs))}
    values = jnp.concatenate([blocks[q] for q in range(slabs)], axis=0)
    pick = one_hot(iota((8 * slabs, LANES), 0).astype(F32) == place_ref[0:1, :])
    found = sum(dot(part, pick, ((0,), (0,))) for part in pieces(values))
    observed_ref[...] = jnp.where(place_ref[1:2, :] > 0.5, found[64:], found[:64])
    traces = jnp.sum(got_ref[pl.ds(8, slabs, stride=9), :], axis=0, keepdims=True)
    total_ref[...] = traces[:, :1] * scale


def call(kernel, inputs, outs, scratch=(), **params):
    kinds = {"v": pltpu.VMEM, "s": pltpu.SMEM, "h": pltpu.HBM, "w": pltpu.VMEM}
    held = {"w": pltpu.VMEM, "h": pltpu.HBM}
    arrays = [pltpu.with_memory_space_constraint(x, held[k]) if k in held else x for k, x in inputs]
    return pl.pallas_call(
        functools.partial(kernel, **params),
        in_specs=[pl.BlockSpec(memory_space=kinds[k]) for k, _ in inputs],
        out_specs=[pl.BlockSpec(memory_space=kinds[k]) for k, _, _ in outs],
        out_shape=[pltpu.VMEM(s, t) if k == "w" else jax.ShapeDtypeStruct(s, t) for k, s, t in outs],
        scratch_shapes=list(scratch),
        compiler_params=pltpu.CompilerParams(vmem_limit_bytes=VMEM_LIMIT),
    )(*arrays)


def body(probe_fields, sensor_rows, sensor_cols, row_frac, col_frac, sensor_weights, owner_order):
    at = lax.axis_index("slab").astype(jnp.int32).reshape(1)
    slabs = lax.axis_size("slab")
    groups = lax.axis_size("probe")
    per_list = slabs * SLOTS
    tiles = probe_fields.shape[2] // LANES
    fields = probe_fields.reshape(16, 4, 4, tiles, LANES).transpose(0, 1, 3, 2, 4)
    flat = [x.reshape(slabs, LANES) for x in (sensor_rows, sensor_cols, row_frac, col_frac, sensor_weights, owner_order)]
    half = per_list // 2
    to_cross, meta, place, flag, lines = call(
        forward_kernel,
        [("s", at)] + [("h", x) for x in flat] + [("h", fields)],
        [("w", (64, per_list), F32), ("w", (16, 2 * per_list), F32), ("w", (8, LANES), F32), ("s", (4,), jnp.int32)]
        + [("w", (16, tiles, 16, LANES), BF16)],
        [
            pltpu.VMEM((3, slabs, LANES), jnp.int32),
            pltpu.VMEM((3, slabs, LANES), F32),
            pltpu.SemaphoreType.DMA((CHUNKS, 4)),
            pltpu.SemaphoreType.DMA((6,)),
        ],
    )
    swap_cross = [(i, i + 1 if i % 2 else i - 1) for i in range(1, slabs - 1)]
    swap_same = [(i, i - 1 if i % 2 else i + 1) for i in range(slabs)]
    cross = lax.ppermute(to_cross, "slab", swap_cross)
    to_same, rest = call(
        rest_kernel,
        [("w", lines), ("w", meta), ("s", flag)],
        [("w", (64, per_list), F32), ("w", (64, half), F32)],
    )
    same = lax.ppermute(to_same, "slab", swap_same)
    blocks, trace, sources = call(
        combine_kernel,
        [("w", x) for x in (rest, to_same, to_cross, same, cross, meta)] + [("s", at)],
        [("w", (8 * slabs, LANES), F32), ("w", (8, LANES), F32), ("w", (256, 2 * per_list), BF16)],
    )
    traces = [trace]
    for k in range(1, groups):
        traces.append(lax.ppermute(trace, "probe", [(i, (i + k) % groups) for i in range(groups)]))
    (send,) = call(pack_kernel, [("w", blocks)] + [("w", x) for x in traces], [("w", (9 * slabs, LANES), F32)])
    got = lax.all_to_all(
        send.reshape(slabs, 1, 9 * LANES), "slab", 0, 0, axis_index_groups=[exchange_order(slabs)], tiled=True
    )
    (out,) = call(
        adjoint_kernel,
        [("w", sources), ("w", meta), ("s", flag)],
        [("h", fields.shape, BF16)],
        [pltpu.VMEM((16, tiles, 16, LANES), BF16), pltpu.SemaphoreType.DMA((OUT_CHUNKS, 4))],
    )
    count = probe_fields.shape[0] * groups * sensor_rows.shape[0]
    observed, total = call(
        finish_kernel,
        [("w", got.reshape(9 * slabs, LANES)), ("w", place)],
        [("v", (64, LANES), F32), ("v", (1, 1), F32)],
        scale=1.0 / count,
    )
    adjoint = out.transpose(0, 1, 3, 2, 4).reshape(probe_fields.shape)
    return adjoint, observed, total.reshape(())


def solution(mesh):
    placed = (P("probe", "slab", None), P(), P(), P(), P(), P(), P())

    return jax.shard_map(
        body,
        mesh=mesh,
        in_specs=placed,
        out_specs=(P("probe", "slab", None), P("probe", "slab"), P()),
        check_vma=False,
    )
```
